16 devices in a mesh: dp: 2 (over y, z), sp: 8 (over x, core).
Axes of the slice: x: 4, y: 2, z: 1, core: 2. Of those that a mesh axis runs over, the one named last changes fastest.
The devices are a block of a 4x4x8 slice.
Arguments:
- x: bfloat16 [8192, 4608], P(('dp', 'sp')), parts along dimension 0
- gain: bfloat16 [4608], replicated
- wq: bfloat16 [4608, 4096], P('sp')
- wk: bfloat16 [4608, 2048], P('sp')
- wv: bfloat16 [4608, 2048], P('sp')
- wo: bfloat16 [4096, 4608], P('sp')
Outputs:
- output: bfloat16 [8192, 4608], P(('dp', 'sp')), parts along dimension 0
There are 2 independent parts. The reference program is written for one: setup_inputs(seed, part) draws one part's arguments, and reference() takes and returns one part's arrays. A program takes and returns all parts, laid end to end along the dimension named above; an argument that names none is the same for every part.
All inputs are finite; a program needn't handle non-finite values.
Results may differ from the reference program's by a relative error of at most 0.012.
Values are sent between devices in bfloat16 or wider.
A program may use at most 768 MiB of HBM per device.

```python
import jax
import jax.numpy as jnp
from jax import lax

ROWS = 4096
D = 4608
HEADS = 32
KV_HEADS = 16
HEAD = 128
THETA = 10000


def setup_inputs(seed: int = 0, part: int = 0) -> dict:
    kx, kn, kq, kk, kv, ko = jax.random.split(jax.random.key(seed), 6)

    def weights(key, rows, columns):
        return jax.random.normal(key, (rows, columns), jnp.float32) * rows**-0.5

    drawn = {
        "x": jax.random.normal(jax.random.fold_in(kx, part), (ROWS, D), jnp.float32),
        "gain": 1 + 0.1 * jax.random.normal(kn, (D,), jnp.float32),
        "wq": 2 * weights(kq, D, HEADS * HEAD),
        "wk": 2 * weights(kk, D, KV_HEADS * HEAD),
        "wv": 4 * weights(kv, D, KV_HEADS * HEAD),
        "wo": weights(ko, HEADS * HEAD, D),
    }
    return {k: v.astype(jnp.bfloat16) for k, v in drawn.items()}


def normed(x, gain):
    wide = x.astype(jnp.float32)
    scale = lax.rsqrt(jnp.mean(wide * wide, -1, keepdims=True) + 1e-6)
    return (wide * scale * gain.astype(jnp.float32)).astype(jnp.bfloat16)


def turned(t, place, theta):
    half = t.shape[-1] // 2
    angle = place.astype(jnp.float32)[:, None] * theta ** (-jnp.arange(half, dtype=jnp.float32) / half)
    cos, sin = jnp.cos(angle)[:, None], jnp.sin(angle)[:, None]
    a, b = t[..., :half].astype(jnp.float32), t[..., half:].astype(jnp.float32)
    return jnp.concatenate([a * cos - b * sin, b * cos + a * sin], -1).astype(jnp.bfloat16)


def matmul(a, w):
    return jnp.dot(a, w, preferred_element_type=jnp.float32).astype(jnp.bfloat16)


def einsum(form, a, b):
    return jnp.einsum(form, a.astype(jnp.float32), b.astype(jnp.float32))


def attention(q, k, v):
    scores = einsum("tgsd,ugd->gstu", q, k) * q.shape[-1] ** -0.5
    token = jnp.arange(q.shape[0])
    scores = jnp.where(token[:, None] >= token, scores, -jnp.inf)
    weights = jax.nn.softmax(scores, -1).astype(jnp.bfloat16)
    return einsum("gstu,ugd->tgsd", weights, v).astype(jnp.bfloat16)


def reference(x, gain, wq, wk, wv, wo):
    a, place = normed(x, gain), jnp.arange(ROWS)
    q = turned(matmul(a, wq).reshape(ROWS, HEADS, HEAD), place, THETA).reshape(ROWS, KV_HEADS, -1, HEAD)
    k = turned(matmul(a, wk).reshape(ROWS, KV_HEADS, HEAD), place, THETA)
    v = matmul(a, wv).reshape(ROWS, KV_HEADS, HEAD)
    seen = attention(q, k, v).reshape(ROWS, HEADS * HEAD)
    return (x.astype(jnp.float32) + jnp.dot(seen, wo, preferred_element_type=jnp.float32)).astype(jnp.bfloat16)
```

```python
import functools

import jax
import jax.numpy as jnp
from jax import lax
from jax.experimental import pallas as pl
from jax.experimental.pallas import tpu as pltpu
from jax.sharding import PartitionSpec as P

HEAD = 128
THETA = 10000
NEG = -1e30
HIDDEN = 2 * NEG
LOG2E = 1.4426950408889634
VMEM = 67043328
MESH = pl.DeviceIdType.MESH
PIECE = 256


def _dot(a, b, ca, cb):
    return lax.dot_general(a, b, (((ca,), (cb,)), ((), ())), preferred_element_type=jnp.float32)


def _kernel(n_sp, x_ref, gain_ref, freq_ref, wq_ref, wk_ref, wv_ref, wo_ref, seen_ref, full_ref,
            a_s, w_s, qkv_s, top_s, mix_s, ss, rs, ls):
    me, group = lax.axis_index("sp"), lax.axis_index("dp")
    chips = n_sp // 2
    c, k = lax.div(me, 2), lax.rem(me, 2)
    half = lax.rem(group, 2)
    pair = {"dp": group + 1 - 2 * half, "sp": me}
    own, depth = x_ref.shape
    wrows = wq_ref.shape[0]
    hrows = wrows // 2
    qc, kc = wq_ref.shape[1] // n_sp, wk_ref.shape[1] // n_sp
    heads, kv_heads = qc // HEAD, kc // HEAD
    orows = wo_ref.shape[0]
    tokens = own * n_sp

    def shard(off, dk=0):
        return lax.rem(c + off, chips) * 2 + lax.rem(k + dk, 2)

    left, right, partner = shard(chips - 1), shard(1), shard(0, 1)
    L, R, O = chips - 1, 1, 2

    ids = {}
    started = []

    def send(name, src, dst, to):
        i = ids.setdefault(name, len(ids))
        copy = pltpu.make_async_remote_copy(src, dst, ss.at[i], rs.at[i], device_id=to if isinstance(to, dict) else {"sp": to},
                                            device_id_type=MESH)
        copy.start()
        started.append((name, copy))

    def recv(name, dst):
        i = ids[name]
        pltpu.make_async_remote_copy(dst, dst, ss.at[i], rs.at[i], device_id={"sp": partner}, device_id_type=MESH).wait_recv()

    def sent(*names):
        for name, copy in list(started):
            if not names or any(name.startswith(n) for n in names):
                copy.wait_send()
                started.remove((name, copy))

    barrier = pltpu.get_barrier_semaphore()
    for off in range(chips):
        for dk in (0, 1):
            if off or dk:
                pl.semaphore_signal(barrier, inc=1, device_id={"sp": shard(off, dk)}, device_id_type=MESH)
    pl.semaphore_signal(barrier, inc=1, device_id=pair, device_id_type=MESH)
    load_x = pltpu.make_async_copy(x_ref, a_s.at[pl.ds(me * own, own)], ls.at[0])
    load_x.start()
    locals_ = []
    spans = ((wq_ref, qc, 0), (wk_ref, kc, qc), (wv_ref, kc, qc + kc))
    for i, (ref, wide, at) in enumerate(spans):
        copy = pltpu.make_async_copy(ref.at[:, pl.ds(pl.multiple_of(me * wide, 128), wide)], w_s.at[pl.ds(me * wrows, wrows), at : at + wide],
                                     ls.at[1 + i])
        copy.start()
        locals_.append(copy)
    pl.semaphore_wait(barrier, n_sp)

    far = [(off, dk) for off in (O, R, L) for dk in (0, 1)]

    def w_rows(s, h):
        return pl.ds(s * wrows + h * hrows, hrows)

    for off, dk in far:
        to = shard(off, dk)
        for i, (ref, wide, at) in enumerate(spans):
            send(f"w{off}{dk}{i}", ref.at[pl.ds(half * hrows, hrows), pl.ds(pl.multiple_of(to * wide, 128), wide)],
                 w_s.at[w_rows(me, half), at : at + wide], to)
    for i, (ref, wide, at) in enumerate(spans):
        send(f"w01{i}", ref.at[:, pl.ds(pl.multiple_of(partner * wide, 128), wide)], w_s.at[pl.ds(me * wrows, wrows), at : at + wide], partner)

    part = orows // 4

    def o_rows(s, h, p):
        return pl.ds(s * orows + (2 * h + p) * part, part)

    def o_half(s, h):
        return pl.ds(s * orows + h * 2 * part, 2 * part)

    for p in (0, 1):
        src = wo_ref.at[pl.ds((2 * half + p) * part, part)]
        send(f"oR{p}", src, full_ref.at[o_rows(me, half, p)], right)
        src = wo_ref.at[pl.ds((2 * half + 1 - p) * part, part)]
        send(f"oL{1 - p}", src, full_ref.at[o_rows(me, half, 1 - p)], left)

    load_x.wait()
    step = 32

    def norm(i, _):
        here = pl.ds(me * own + i * step, step)
        wide = a_s[here, :].astype(jnp.float32)
        scale = lax.rsqrt(jnp.mean(wide * wide, -1, keepdims=True) + 1e-6)
        a_s[here, :] = (wide * scale * gain_ref[...].astype(jnp.float32)).astype(jnp.bfloat16)

    lax.fori_loop(0, own // step, norm, None)
    xh = own // 2

    def x_rows(s, p):
        return pl.ds(s * own + p * xh, xh)

    for p in (0, 1):
        send(f"xR{p}", a_s.at[x_rows(me, p)], a_s.at[x_rows(me, p)], right)
        send(f"xL{1 - p}", a_s.at[x_rows(me, 1 - p)], a_s.at[x_rows(me, 1 - p)], left)
    send("xP", a_s.at[pl.ds(me * own, own)], a_s.at[pl.ds(me * own, own)], partner)

    for off, dk in far:
        src = shard(chips - off, dk)
        for i, (ref, wide, at) in enumerate(spans):
            recv(f"w{off}{dk}{i}", w_s.at[w_rows(src, half), at : at + wide])
        send(f"g{off}{dk}", w_s.at[w_rows(src, half)], w_s.at[w_rows(src, half)], pair)
    for i, (ref, wide, at) in enumerate(spans):
        recv(f"w01{i}", w_s.at[pl.ds(partner * wrows, wrows), at : at + wide])
    for copy in locals_:
        copy.wait()
    for off, dk in far:
        src = shard(chips - off, dk)
        recv(f"g{off}{dk}", w_s.at[w_rows(src, 1 - half)])

    first_half = lax.broadcasted_iota(jnp.int32, (PIECE, HEAD), 1) < HEAD // 2

    def project(start, count):
        def piece(i, _):
            at = start + i * PIECE
            here = pl.ds(at, PIECE)
            place = (at + lax.broadcasted_iota(jnp.int32, (PIECE, HEAD), 0)).astype(jnp.float32)
            angle = place * freq_ref[...]
            cos, sin = jnp.cos(angle), jnp.sin(angle)
            sin = jnp.where(first_half, -sin, sin)

            def columns(n, _):
                there = pl.ds(pl.multiple_of(n * 2 * HEAD, 2 * HEAD), 2 * HEAD)
                got = _dot(a_s[here, :], w_s[:, there], 1, 0).astype(jnp.bfloat16).astype(jnp.float32)
                turn = n * 2 * HEAD < qc + kc
                cn, sn = jnp.where(turn, cos, 1.0), jnp.where(turn, sin, 0.0)
                two = [got[:, :HEAD], got[:, HEAD:]]
                two = [t * cn + pltpu.roll(t, HEAD // 2, 1) * sn for t in two]
                qkv_s[here, there] = jnp.concatenate(two, 1).astype(jnp.bfloat16)

            lax.fori_loop(0, (qc + 2 * kc) // (2 * HEAD), columns, None)

        lax.fori_loop(0, count, piece, None)

    whole, bit = own // PIECE, xh // PIECE
    project(me * own, whole)
    recv("xP", a_s.at[pl.ds(partner * own, own)])
    project(partner * own, whole)

    sl, sr, so = shard(L), shard(R), shard(O)
    pl_, pr, po = shard(L, 1), shard(R, 1), shard(O, 1)

    def wo_on(name, s, p):
        send(f"og{name}", full_ref.at[o_rows(s, half, p)], full_ref.at[o_rows(s, half, p)], pair)
        send(f"od{name}", full_ref.at[o_rows(s, half, p)], full_ref.at[o_rows(s, half, p)], partner)

    for p in (0, 1):
        recv(f"oR{p}", full_ref.at[o_rows(sl, half, p)])
        wo_on(f"L{p}", sl, p)
        recv(f"oL{1 - p}", full_ref.at[o_rows(sr, half, 1 - p)])
        wo_on(f"R{1 - p}", sr, 1 - p)
    send("oP", wo_ref, full_ref.at[pl.ds(me * orows, orows)], partner)

    for p in (0, 1):
        recv(f"xR{p}", a_s.at[x_rows(sl, p)])
        if p == 0:
            send("xfR", a_s.at[x_rows(sl, p)], a_s.at[x_rows(sl, p)], right)
        send(f"xpL{p}", a_s.at[x_rows(sl, p)], a_s.at[x_rows(sl, p)], partner)
        recv(f"xL{1 - p}", a_s.at[x_rows(sr, 1 - p)])
        if p == 0:
            send("xfL", a_s.at[x_rows(sr, 1 - p)], a_s.at[x_rows(sr, 1 - p)], left)
        send(f"xpR{1 - p}", a_s.at[x_rows(sr, 1 - p)], a_s.at[x_rows(sr, 1 - p)], partner)
        if p == 0:
            send("ofR", full_ref.at[o_rows(sl, half, 0)], full_ref.at[o_rows(sl, half, 0)], right)
            send("ofL", full_ref.at[o_rows(sr, half, 1)], full_ref.at[o_rows(sr, half, 1)], left)
        project(sl * own + p * xh, bit)
        project(sr * own + (1 - p) * xh, bit)
        recv(f"xpL{p}", a_s.at[x_rows(pl_, p)])
        project(pl_ * own + p * xh, bit)
        recv(f"xpR{1 - p}", a_s.at[x_rows(pr, 1 - p)])
        project(pr * own + (1 - p) * xh, bit)
    recv("xfR", a_s.at[x_rows(so, 0)])
    send("xpO0", a_s.at[x_rows(so, 0)], a_s.at[x_rows(so, 0)], partner)
    recv("xfL", a_s.at[x_rows(so, 1)])
    send("xpO1", a_s.at[x_rows(so, 1)], a_s.at[x_rows(so, 1)], partner)
    project(so * own, whole)
    recv("xpO0", a_s.at[x_rows(po, 0)])
    recv("xpO1", a_s.at[x_rows(po, 1)])
    project(po * own, whole)
    sent("x")

    keep_wo = pltpu.make_async_copy(wo_ref, a_s.at[pl.ds(me * own, own)], ls.at[0])
    keep_wo.start()

    scale = HEAD**-0.5
    e = scale * LOG2E
    share = heads // kv_heads
    ones = jnp.ones((8, own), jnp.bfloat16)
    dv = HEAD

    def attend(i):
        rows = pl.ds(i * own, own)
        top_s[...] = jnp.full(top_s.shape, NEG, jnp.float32)
        mix_s[...] = jnp.zeros(mix_s.shape, jnp.float32)

        def block(j, masked):
            keys = pl.ds(j * own, own)
            scores = []
            for h in range(heads):
                at = qc + (h // share) * HEAD
                scores.append(_dot(qkv_s[keys, at : at + HEAD], qkv_s[rows, h * HEAD : (h + 1) * HEAD], 1, 1))
            if masked:
                ok = lax.broadcasted_iota(jnp.int32, (own, own), 1) >= lax.broadcasted_iota(jnp.int32, (own, own), 0)
            weights, keeps = [], []
            for h, s in enumerate(scores):
                if masked:
                    s = jnp.where(ok, s, HIDDEN)
                old = top_s[h : h + 1, :]
                top = jnp.maximum(old, s.max(axis=0, keepdims=True))
                top_s[h : h + 1, :] = top
                weights.append(jnp.exp2((s - top) * e).astype(jnp.bfloat16))
                keeps.append(jnp.exp2((old - top) * e))
            for h, (p, keep) in enumerate(zip(weights, keeps)):
                at = qc + kc + (h // share) * HEAD
                values = jnp.concatenate([qkv_s[keys, at : at + HEAD].T, ones], axis=0)
                mix_s[h] = mix_s[h] * keep + _dot(values, p, 1, 0)

        lax.fori_loop(0, i, lambda j, _: block(j, False), None)
        block(i, True)
        for h in range(heads):
            a_s[rows, h * HEAD : (h + 1) * HEAD] = (mix_s[h, :dv, :] * (1 / mix_s[h, dv : dv + 1, :])).T.astype(jnp.bfloat16)

    base = len(ids)
    for i in range(n_sp - 1):
        ids[f"seen{i}"] = base + i

    def seen_copy(t, to, src):
        return pltpu.make_async_remote_copy(a_s.at[pl.ds(to * own, own), :qc], seen_ref.at[:, pl.ds(pl.multiple_of(src * qc, 128), qc)],
                                            ss.at[base + t], rs.at[base + t], device_id={"sp": to}, device_id_type=MESH)

    def place_of(t):
        return chips - 1 - lax.div(t, 2), 1 - lax.rem(t, 2)

    def attention(t, _):
        off, dk = place_of(t)
        to = shard(off, dk)
        attend(to)
        seen_copy(t, to, me).start()

    early = chips
    lax.fori_loop(0, early, attention, None)
    keep_wo.wait()
    put_wo = pltpu.make_async_copy(a_s.at[pl.ds(me * own, own)], full_ref.at[pl.ds(me * orows, orows)], ls.at[1])
    put_wo.start()
    recv("ofR", full_ref.at[o_rows(so, half, 0)])
    wo_on("O0", so, 0)
    recv("ofL", full_ref.at[o_rows(so, half, 1)])
    wo_on("O1", so, 1)
    other = 1 - half

    def wo_over(name, s, p):
        recv(f"og{name}", full_ref.at[o_rows(s, other, p)])
        send(f"oe{name}", full_ref.at[o_rows(s, other, p)], full_ref.at[o_rows(s, other, p)], partner)

    for p in (0, 1):
        wo_over(f"L{p}", sl, p)
        wo_over(f"R{1 - p}", sr, 1 - p)
    lax.fori_loop(early, n_sp - 1, attention, None)
    put_wo.wait()
    attend(me)
    mine = pltpu.make_async_copy(a_s.at[pl.ds(me * own, own), :qc], seen_ref.at[:, pl.ds(pl.multiple_of(me * qc, 128), qc)], ls.at[0])
    mine.start()
    for p in (0, 1):
        wo_over(f"O{p}", so, p)

    def finish(t, _):
        off, dk = place_of(t)
        copy = seen_copy(t, shard(off, dk), shard(chips - off, dk))
        copy.wait_send()
        copy.wait_recv()

    lax.fori_loop(0, n_sp - 1, finish, None)
    mine.wait()
    for s, name in ((pl_, "L"), (pr, "R"), (po, "O")):
        for p in (0, 1):
            recv(f"od{name}{p}", full_ref.at[o_rows(s, half, p)])
            recv(f"oe{name}{p}", full_ref.at[o_rows(s, other, p)])
    recv("oP", full_ref.at[pl.ds(partner * orows, orows)])
    sent()


def solution(mesh):
    n_sp = mesh.shape["sp"]

    def step(x, gain, wq, wk, wv, wo):
        own, depth = x.shape
        tokens = own * n_sp
        columns = (wq.shape[1] + wk.shape[1] + wv.shape[1]) // n_sp
        half = HEAD // 2
        freq = THETA ** (-jnp.arange(half, dtype=jnp.float32) / half)
        freq = jnp.concatenate([freq, freq])[None]
        heads = wq.shape[1] // n_sp // HEAD
        hbm, vmem = pl.BlockSpec(memory_space=pltpu.HBM), pl.BlockSpec(memory_space=pltpu.VMEM)
        seen, full = pl.pallas_call(
            functools.partial(_kernel, n_sp),
            out_shape=[jax.ShapeDtypeStruct((own, wq.shape[1]), jnp.bfloat16),
                       jax.ShapeDtypeStruct((wo.shape[0] * n_sp, wo.shape[1]), jnp.bfloat16)],
            in_specs=[hbm, vmem, vmem, hbm, hbm, hbm, hbm],
            out_specs=[hbm, hbm],
            scratch_shapes=[
                pltpu.VMEM((tokens, depth), jnp.bfloat16),
                pltpu.VMEM((wq.shape[0] * n_sp, columns), jnp.bfloat16),
                pltpu.VMEM((tokens, columns), jnp.bfloat16),
                pltpu.VMEM((heads, own), jnp.float32),
                pltpu.VMEM((heads, HEAD + 8, own), jnp.float32),
                pltpu.SemaphoreType.DMA((96,)),
                pltpu.SemaphoreType.DMA((96,)),
                pltpu.SemaphoreType.DMA((4,)),
            ],
            compiler_params=pltpu.CompilerParams(collective_id=0, has_side_effects=True, vmem_limit_bytes=VMEM),
        )(x, gain[None], freq, wq, wk, wv, wo)
        y = jnp.dot(seen, full, preferred_element_type=jnp.float32)
        return (x.astype(jnp.float32) + y).astype(jnp.bfloat16)

    tokens, whole = P(("dp", "sp"), None), P("sp", None)
    return jax.shard_map(
        step,
        mesh=mesh,
        in_specs=(tokens, P(None), whole, whole, whole, whole),
        out_specs=tokens,
        check_vma=False,
    )
```

```python
import functools

import jax
import jax.numpy as jnp
from jax import lax
from jax.experimental import pallas as pl
from jax.experimental.pallas import tpu as pltpu
from jax.sharding import PartitionSpec as P

HEAD = 128
THETA = 10000
NEG = -1e30
HIDDEN = 2 * NEG
LOG2E = 1.4426950408889634
VMEM = 67043328
MESH = pl.DeviceIdType.MESH
WIDE = 768


def _dot(a, b, ca, cb):
    return lax.dot_general(a, b, (((ca,), (cb,)), ((), ())), preferred_element_type=jnp.float32)


def _kernel(n_sp, x_ref, gain_ref, freq_ref, wq_ref, wk_ref, wv_ref, wo_ref, y_ref, full_ref,
            a_s, w_s, q_s, kv_s, seen_s, top_s, mix_s, ss, rs, ls):
    me, group = lax.axis_index("sp"), lax.axis_index("dp")
    chips = n_sp // 2
    c, k = lax.div(me, 2), lax.rem(me, 2)
    half = lax.rem(group, 2)
    other = 1 - half
    pair = {"dp": group + 1 - 2 * half, "sp": me}
    own, depth = x_ref.shape
    wrows = wq_ref.shape[0]
    hrows = wrows // 2
    orows = wo_ref.shape[0]
    units = chips
    qc, kc = wq_ref.shape[1] // units, wk_ref.shape[1] // units
    two = 2 * own

    mate, mirror = c + 1 - 2 * lax.rem(c, 2), chips - 1 - c
    across = chips - 1 - mate
    chip = {"S": c, "K": mate, "T": mirror, "O": across}

    def device(name, dk=0):
        return chip[name] * 2 + lax.rem(k + dk, 2)

    def unit(name, dk=0):
        return lax.div(chip[name], chips // 2) * 2 + lax.rem(k + dk, 2)

    partner = device("S", 1)
    unit_here = unit("S")

    ids = {}
    started = []

    def copy_of(name, src, dst, to):
        i = ids.setdefault(name, len(ids))
        return pltpu.make_async_remote_copy(src, dst, ss.at[i], rs.at[i], device_id=to if isinstance(to, dict) else {"sp": to},
                                            device_id_type=MESH)

    def send(name, src, dst, to, when=None):
        copy = copy_of(name, src, dst, to)
        if when is None:
            copy.start()
        else:
            pl.when(when)(copy.start)
        started.append((name, copy, when))

    def recv(name, dst, when=None):
        with jax.named_scope(f"recv_{name}"):
            copy = copy_of(name, dst, dst, partner)
            if when is None:
                copy.wait_recv()
            else:
                pl.when(when)(copy.wait_recv)

    def sent(*names):
        with jax.named_scope("sent"):
            for entry in list(started):
                name, copy, when = entry
                if not names or any(name.startswith(n) for n in names):
                    if when is None:
                        copy.wait_send()
                    else:
                        pl.when(when)(copy.wait_send)
                    started.remove(entry)

    barrier = pltpu.get_barrier_semaphore()
    for name in "SKTO":
        for dk in (0, 1):
            if (name, dk) != ("S", 0):
                pl.semaphore_signal(barrier, inc=1, device_id={"sp": device(name, dk)}, device_id_type=MESH)
    pl.semaphore_signal(barrier, inc=1, device_id=pair, device_id_type=MESH)
    here_own = pl.ds(k * own, own)
    load_x = pltpu.make_async_copy(x_ref, a_s.at[here_own], ls.at[0])
    load_x.start()
    spans = ((wk_ref, kc, 0), (wv_ref, kc, kc), (wq_ref, qc, 2 * kc))
    parts = {"v": (0, 2 * kc), "q": (2 * kc, qc)}
    own_weights = []
    for i, (ref, wide, at) in enumerate(spans):
        copy = pltpu.make_async_copy(ref.at[:, pl.ds(pl.multiple_of(unit_here * wide, 128), wide)],
                                     w_s.at[pl.ds(me * wrows, wrows), at : at + wide], ls.at[1 + i])
        copy.start()
        own_weights.append(copy)
    with jax.named_scope("k_barrier"):
        pl.semaphore_wait(barrier, n_sp)

    def w_rows(s, h):
        return pl.ds(s * wrows + h * hrows, hrows)

    for i, (ref, wide, at) in enumerate(spans):
        for name in "TK":
            for dk in (0, 1):
                columns = pl.ds(pl.multiple_of(unit(name, dk) * wide, 128), wide)
                send(f"w{name}{dk}{i}", ref.at[pl.ds(half * hrows, hrows), columns], w_s.at[w_rows(me, half), at : at + wide],
                     device(name, dk))
        columns = pl.ds(pl.multiple_of(unit("S", 1) * wide, 128), wide)
        send(f"wP{i}", ref.at[:, columns], w_s.at[pl.ds(me * wrows, wrows), at : at + wide], partner)

    load_x.wait()
    step = 32

    def norm(i, _):
        here = pl.ds(k * own + i * step, step)
        wide = a_s[here, :].astype(jnp.float32)
        scale = lax.rsqrt(jnp.mean(wide * wide, -1, keepdims=True) + 1e-6)
        a_s[here, :] = (wide * scale * gain_ref[...].astype(jnp.float32)).astype(jnp.bfloat16)

    with jax.named_scope("norm"):
        lax.fori_loop(0, own // step, norm, None)
    xh = own // 2
    for p in (0, 1):
        src = a_s.at[pl.ds(k * own + p * xh, xh)]
        send(f"xT{p}", src, a_s.at[pl.ds(two + k * own + p * xh, xh)], device("T"))
    send("xP", a_s.at[here_own], a_s.at[here_own], partner)

    oh, oc = orows // 2, depth // 2

    def o_at(s, h, p):
        return full_ref.at[pl.ds(s * orows + h * oh, oh), p * oc : (p + 1) * oc]

    def o_send(name, p):
        send(f"o{name}{p}", wo_ref.at[pl.ds(half * oh, oh), p * oc : (p + 1) * oc], o_at(me, half, p), device(name))

    o_send("T", 0)
    o_send("T", 1)

    def w_in(name, part):
        for dk in (0, 1):
            for i, (_, wide, at) in enumerate(spans):
                if (part == "q") == (i == 2):
                    recv(f"w{name}{dk}{i}", w_s.at[w_rows(device(name, dk), half), at : at + wide])

    def w_block(name, dk, h, part):
        at, wide = parts[part]
        return w_s.at[w_rows(device(name, dk), h), at : at + wide]

    def w_on(name, part, to):
        for dk in (0, 1):
            block = w_block(name, dk, half, part)
            if to == "K":
                send(f"wO{dk}{part}", block, block, device("K"))
            else:
                send(f"g{name}{dk}{part}", block, block, pair)

    def w_across(part):
        for dk in (0, 1):
            recv(f"wO{dk}{part}", w_block("O", dk, half, part))

    w_in("T", "v")
    w_on("T", "v", "K")
    w_on("T", "v", "pair")
    w_in("K", "v")
    w_on("K", "v", "pair")
    w_in("T", "q")
    w_on("T", "q", "K")
    o_send("K", 0)
    w_across("v")
    w_on("O", "v", "pair")
    w_in("K", "q")
    w_on("T", "q", "pair")
    w_on("K", "q", "pair")
    w_across("q")
    w_on("O", "q", "pair")

    def w_ready(part):
        for i, (_, wide, at) in enumerate(spans):
            if (part == "q") == (i == 2):
                recv(f"wP{i}", w_s.at[pl.ds(partner * wrows, wrows), at : at + wide])
                own_weights[i].wait()
        for name in "TKO":
            for dk in (0, 1):
                recv(f"g{name}{dk}{part}", w_block(name, dk, other, part))

    first_half = lax.broadcasted_iota(jnp.int32, (own, HEAD), 1) < HEAD // 2
    pairs = kc // (2 * HEAD)
    pw = 2 * HEAD

    def rotation(place):
        angle = (place + lax.broadcasted_iota(jnp.int32, (own, HEAD), 0)).astype(jnp.float32) * freq_ref[...]
        cos, sin = jnp.cos(angle), jnp.sin(angle)
        return cos, jnp.where(first_half, -sin, sin)

    def product(rows, at):
        return _dot(a_s[rows, :], w_s[:, pl.ds(pl.multiple_of(at, pw), pw)], 1, 0).astype(jnp.bfloat16)

    def turned(got, cos, sin):
        wide = got.astype(jnp.float32)
        heads = [wide[:, :HEAD], wide[:, HEAD:]]
        return jnp.concatenate([t * cos + pltpu.roll(t, HEAD // 2, 1) * sin for t in heads], 1).astype(jnp.bfloat16)

    def place_of(slot, core):
        return ((c if slot == 0 else mirror) * 2 + core) * own

    def project_kv(slot, core):
        rows, place = pl.ds(slot * two + core * own, own), place_of(slot, core)
        with jax.named_scope("project_kv"):
            cos, sin = rotation(place)

            def one(b, _):
                kv_s[b, pl.ds(place, own), :pw] = turned(product(rows, b * pw), cos, sin)
                kv_s[b, pl.ds(place, own), pw:] = product(rows, kc + b * pw)

            lax.fori_loop(0, pairs, one, None)

    def project_q():
        with jax.named_scope("project_q"):

            def some(i, _):
                slot, core = lax.div(i, 2), lax.rem(i, 2)
                rows = pl.ds(i * own, own)
                cos, sin = rotation((jnp.where(slot == 0, c, mirror) * 2 + core) * own)

                def one(b, _):
                    for j in (0, 1):
                        q_s[b, rows, j * pw : (j + 1) * pw] = turned(product(rows, 2 * kc + (2 * b + j) * pw), cos, sin)

                lax.fori_loop(0, pairs, one, None)

            lax.fori_loop(0, 4, some, None)

    def kv_rows(chunk):
        return kv_s.at[:, pl.ds(chunk * two, two), :]

    def kv_send(slot):
        chunk = c if slot == 0 else mirror
        send(f"kv{slot}", kv_rows(chunk), kv_rows(chunk), device("K"), when=chunk < chips - 1)

    def wo_on(name, p):
        piece = o_at(device(name), half, p)
        send(f"og{name}{p}", piece, piece, pair)
        send(f"od{name}{p}", piece, piece, partner)

    def wo_over(name, p):
        piece = o_at(device(name), other, p)
        recv(f"og{name}{p}", piece)
        send(f"oe{name}{p}", piece, piece, partner)

    w_ready("v")
    recv("xP", a_s.at[pl.ds((1 - k) * own, own)])
    project_kv(0, k)
    project_kv(0, 1 - k)
    kv_send(0)
    recv("oK0", o_at(device("K"), half, 0))
    send("oOT", o_at(device("K"), half, 0), o_at(device("K"), half, 0), device("T"))
    wo_on("K", 0)
    send("oP", wo_ref, full_ref.at[pl.ds(me * orows, orows)], partner)
    for p in (0, 1):
        got = a_s.at[pl.ds(two + k * own + p * xh, xh)]
        recv(f"xT{p}", got)
        send(f"xp{p}", got, got, partner)
    project_kv(1, k)
    for p in (0, 1):
        recv(f"xp{p}", a_s.at[pl.ds(two + (1 - k) * own + p * xh, xh)])
    project_kv(1, 1 - k)
    kv_send(1)
    o_send("K", 1)
    recv("oT0", o_at(device("T"), half, 0))
    wo_on("T", 0)
    w_ready("q")
    project_q()
    recv("oT1", o_at(device("T"), half, 1))
    send("oOK", o_at(device("T"), half, 1), o_at(device("T"), half, 1), device("K"))
    wo_on("T", 1)
    wo_over("K", 0)
    wo_over("T", 0)
    sent("x", "g", "w")
    keep_wo = pltpu.make_async_copy(wo_ref, a_s.at[pl.ds(2 * own, own)], ls.at[0])
    keep_wo.start()
    load_x = pltpu.make_async_copy(x_ref, a_s.at[pl.ds(0, own)], ls.at[1])
    load_x.start()
    recv("kv0", kv_rows(mate), when=mate < chips - 1)
    recv("kv1", kv_rows(across), when=across < chips - 1)

    scale = HEAD**-0.5
    e = scale * LOG2E
    heads, share = 4, 2
    ones = jnp.ones((8, own), jnp.bfloat16)
    dv = HEAD

    def attend(slot, core, b):
        rows = pl.ds(slot * two + core * own, own)
        block_here = jnp.where(slot == 0, c, mirror) * 2 + core
        top_s[...] = jnp.full(top_s.shape, NEG, jnp.float32)
        mix_s[...] = jnp.zeros(mix_s.shape, jnp.float32)

        def block(j, masked):
            keys = pl.ds(j * own, own)
            scores = []
            for h in range(heads):
                at = (h // share) * HEAD
                scores.append(_dot(kv_s[b, keys, at : at + HEAD], q_s[b, rows, h * HEAD : (h + 1) * HEAD], 1, 1))
            if masked:
                ok = lax.broadcasted_iota(jnp.int32, (own, own), 1) >= lax.broadcasted_iota(jnp.int32, (own, own), 0)
            weights, keeps = [], []
            for h, s in enumerate(scores):
                if masked:
                    s = jnp.where(ok, s, HIDDEN)
                old = top_s[h : h + 1, :]
                top = jnp.maximum(old, s.max(axis=0, keepdims=True))
                top_s[h : h + 1, :] = top
                weights.append(jnp.exp2((s - top) * e).astype(jnp.bfloat16))
                keeps.append(jnp.exp2((old - top) * e))
            for h, (p, keep) in enumerate(zip(weights, keeps)):
                at = pw + (h // share) * HEAD
                values = jnp.concatenate([kv_s[b, keys, at : at + HEAD].T, ones], axis=0)
                mix_s[h] = mix_s[h] * keep + _dot(values, p, 1, 0)

        lax.fori_loop(0, block_here, lambda j, _: block(j, False), None)
        block(block_here, True)
        for h in range(heads):
            q_s[b, rows, h * HEAD : (h + 1) * HEAD] = (mix_s[h, :dv, :] * (1 / mix_s[h, dv : dv + 1, :])).T.astype(jnp.bfloat16)

    hc = heads * HEAD
    base = len(ids)
    for i in range(6):
        ids[f"seen{i}"] = base + i

    def spot(t):
        slot = 1 - lax.div(t, 4)
        core = lax.rem(k + lax.rem(lax.div(t, 2) + slot * 1 + (1 - slot) * 1, 2), 2)
        return slot, core, lax.rem(t, 2)

    def seen_copy(t, to, src_unit, rows, b):
        return pltpu.make_async_remote_copy(q_s.at[b, rows], seen_s.at[:, pl.ds(pl.multiple_of(src_unit * qc + b * hc, 128), hc)],
                                            ss.at[base + t], rs.at[base + t], device_id={"sp": to}, device_id_type=MESH)

    def attention(t, _):
        slot, core, b = spot(t)
        with jax.named_scope("attend"):
            attend(slot, core, b)
        to = jnp.where(slot == 0, c, mirror) * 2 + core
        seen_copy(t, to, unit_here, pl.ds(slot * two + core * own, own), b).start()

    lax.fori_loop(0, 3, attention, None)
    keep_wo.wait()
    put_wo = pltpu.make_async_copy(a_s.at[pl.ds(2 * own, own)], full_ref.at[pl.ds(me * orows, orows)], ls.at[0])
    put_wo.start()
    recv("oOT", o_at(device("O"), half, 0))
    wo_on("O", 0)
    recv("oK1", o_at(device("K"), half, 1))
    wo_on("K", 1)
    wo_over("T", 1)
    lax.fori_loop(3, 6, attention, None)
    recv("oOK", o_at(device("O"), half, 1))
    wo_on("O", 1)
    put_wo.wait()
    wo_over("O", 0)
    mine = []

    def attention_here(b, _):
        with jax.named_scope("attend"):
            attend(0, k, b)

    lax.fori_loop(0, 2, attention_here, None)
    for b in (0, 1):
        copy = pltpu.make_async_copy(q_s.at[b, here_own], seen_s.at[:, pl.ds(pl.multiple_of(unit_here * qc + b * hc, 128), hc)], ls.at[2 + b])
        copy.start()
        mine.append(copy)

    with jax.named_scope("finish"):
        for t in range(6):
            slot, core, b = spot(t)
            to = jnp.where(slot == 0, c, mirror) * 2 + core
            copy = seen_copy(t, to, unit_here, pl.ds(slot * two + core * own, own), b)
            copy.wait_send()
            name, dk = ("T", (t // 2 + 1) % 2) if t < 4 else ("S", 1)
            seen_copy(t, partner, unit(name, dk), pl.ds(0, own), b).wait_recv()
        for copy in mine:
            copy.wait()
        load_x.wait()

    def o_ready(p):
        for name in "KTO":
            s = device(name, 1)
            recv(f"od{name}{p}", o_at(s, half, p))
            recv(f"oe{name}{p}", o_at(s, other, p))

    tiles = depth // WIDE

    def fetch(n):
        slot = lax.rem(n, 2)
        columns = pl.ds(pl.multiple_of(slot * WIDE, 128), WIDE)
        return pltpu.make_async_copy(full_ref.at[:, pl.ds(pl.multiple_of(n * WIDE, 128), WIDE)],
                                     w_s.at[pl.ds(0, full_ref.shape[0]), columns], ls.at[4 + slot])

    def put(n):
        columns = pl.ds(pl.multiple_of(n * WIDE, 128), WIDE)
        return pltpu.make_async_copy(a_s.at[pl.ds(own, own), columns], y_ref.at[:, columns], ls.at[6])

    def outputs(first, last):
        def tile(n, _):
            @pl.when(n + 1 < last)
            def _():
                fetch(n + 1).start()

            fetch(n).wait()
            columns = pl.ds(pl.multiple_of(n * WIDE, 128), WIDE)
            slot = pl.ds(pl.multiple_of(lax.rem(n, 2) * WIDE, 128), WIDE)
            got = _dot(seen_s[...], w_s[pl.ds(0, full_ref.shape[0]), slot], 1, 0)
            a_s[pl.ds(own, own), columns] = (a_s[pl.ds(0, own), columns].astype(jnp.float32) + got).astype(jnp.bfloat16)

        fetch(first).start()
        with jax.named_scope("outputs"):
            lax.fori_loop(first, last, tile, None)

    recv("oP", full_ref.at[pl.ds(partner * orows, orows)])
    o_ready(0)
    outputs(0, tiles // 2)
    for name in "KO":
        wo_over(name, 1)
    o_ready(1)
    outputs(tiles // 2, tiles)
    out = pltpu.make_async_copy(a_s.at[pl.ds(own, own)], y_ref, ls.at[6])
    out.start()
    sent()
    out.wait()


def solution(mesh):
    n_sp = mesh.shape["sp"]

    def step(x, gain, wq, wk, wv, wo):
        own, depth = x.shape
        units = n_sp // 2
        columns = (wq.shape[1] + wk.shape[1] + wv.shape[1]) // units
        half = HEAD // 2
        freq = THETA ** (-jnp.arange(half, dtype=jnp.float32) / half)
        freq = jnp.concatenate([freq, freq])[None]
        kc = wk.shape[1] // units
        pairs = kc // (2 * HEAD)
        hbm, vmem = pl.BlockSpec(memory_space=pltpu.HBM), pl.BlockSpec(memory_space=pltpu.VMEM)
        y, _ = pl.pallas_call(
            functools.partial(_kernel, n_sp),
            out_shape=[jax.ShapeDtypeStruct((own, depth), jnp.bfloat16),
                       jax.ShapeDtypeStruct((wo.shape[0] * n_sp, depth), jnp.bfloat16)],
            in_specs=[hbm, vmem, vmem, hbm, hbm, hbm, hbm],
            out_specs=[hbm, hbm],
            scratch_shapes=[
                pltpu.VMEM((4 * own, depth), jnp.bfloat16),
                pltpu.VMEM((wq.shape[0] * n_sp, columns), jnp.bfloat16),
                pltpu.VMEM((pairs, 4 * own, 4 * HEAD), jnp.bfloat16),
                pltpu.VMEM((pairs, own * n_sp, 4 * HEAD), jnp.bfloat16),
                pltpu.VMEM((own, wq.shape[1]), jnp.bfloat16),
                pltpu.VMEM((4, own), jnp.float32),
                pltpu.VMEM((4, HEAD + 8, own), jnp.float32),
                pltpu.SemaphoreType.DMA((80,)),
                pltpu.SemaphoreType.DMA((80,)),
                pltpu.SemaphoreType.DMA((8,)),
            ],
            compiler_params=pltpu.CompilerParams(collective_id=0, has_side_effects=True, vmem_limit_bytes=VMEM),
        )(x, gain[None], freq, wq, wk, wv, wo)
        return y

    tokens, whole = P(("dp", "sp"), None), P("sp", None)
    return jax.shard_map(
        step,
        mesh=mesh,
        in_specs=(tokens, P(None), whole, whole, whole, whole),
        out_specs=tokens,
        check_vma=False,
    )
```

```python
import functools

import jax
import jax.numpy as jnp
from jax import lax
from jax.experimental import pallas as pl
from jax.experimental.pallas import tpu as pltpu
from jax.sharding import PartitionSpec as P

HEAD = 128
THETA = 10000
NEG = -1e30
HIDDEN = 2 * NEG
LOG2E = 1.4426950408889634
VMEM = 67043328
MESH = pl.DeviceIdType.MESH
WIDE = 512


def _dot(a, b, ca, cb):
    return lax.dot_general(a, b, (((ca,), (cb,)), ((), ())), preferred_element_type=jnp.float32)


def _kernel(n_sp, x_ref, gain_ref, freq_ref, wq_ref, wk_ref, wv_ref, wo_ref, y_ref, full_ref,
            a_s, w_s, q_s, kv_s, seen_s, top_s, mix_s, ss, rs, ls):
    me, group = lax.axis_index("sp"), lax.axis_index("dp")
    chips = n_sp // 2
    c, k = lax.div(me, 2), lax.rem(me, 2)
    half = lax.rem(group, 2)
    other = 1 - half
    pair = {"dp": group + 1 - 2 * half, "sp": me}
    own, depth = x_ref.shape
    wrows = wq_ref.shape[0]
    hrows = wrows // 2
    orows = wo_ref.shape[0]
    units = chips
    qc, kc = wq_ref.shape[1] // units, wk_ref.shape[1] // units
    two = 2 * own

    mate, mirror = c + 1 - 2 * lax.rem(c, 2), chips - 1 - c
    across = chips - 1 - mate
    chip = {"S": c, "K": mate, "T": mirror, "O": across}

    def device(name, dk=0):
        return chip[name] * 2 + lax.rem(k + dk, 2)

    def unit(name, dk=0):
        return lax.div(chip[name], chips // 2) * 2 + lax.rem(k + dk, 2)

    partner = device("S", 1)
    unit_here = unit("S")

    ids = {}
    started = []

    def copy_of(name, src, dst, to):
        i = ids.setdefault(name, len(ids))
        return pltpu.make_async_remote_copy(src, dst, ss.at[i], rs.at[i], device_id=to if isinstance(to, dict) else {"sp": to},
                                            device_id_type=MESH)

    def send(name, src, dst, to, when=None):
        copy = copy_of(name, src, dst, to)
        if when is None:
            copy.start()
        else:
            pl.when(when)(copy.start)
        started.append((name, copy, when))

    def recv(name, dst, when=None):
        with jax.named_scope(f"recv_{name}"):
            copy = copy_of(name, dst, dst, partner)
            if when is None:
                copy.wait_recv()
            else:
                pl.when(when)(copy.wait_recv)

    def sent(*names):
        with jax.named_scope("sent"):
            for entry in list(started):
                name, copy, when = entry
                if not names or any(name.startswith(n) for n in names):
                    if when is None:
                        copy.wait_send()
                    else:
                        pl.when(when)(copy.wait_send)
                    started.remove(entry)

    barrier = pltpu.get_barrier_semaphore()
    for name in "SKTO":
        for dk in (0, 1):
            if (name, dk) != ("S", 0):
                pl.semaphore_signal(barrier, inc=1, device_id={"sp": device(name, dk)}, device_id_type=MESH)
    pl.semaphore_signal(barrier, inc=1, device_id=pair, device_id_type=MESH)
    here_own = pl.ds(k * own, own)
    load_x = pltpu.make_async_copy(x_ref, a_s.at[here_own], ls.at[0])
    load_x.start()
    spans = ((wk_ref, kc, 0), (wv_ref, kc, kc), (wq_ref, qc, 2 * kc))
    own_weights = []
    for i, (ref, wide, at) in enumerate(spans):
        copy = pltpu.make_async_copy(ref.at[:, pl.ds(pl.multiple_of(unit_here * wide, 128), wide)],
                                     w_s.at[pl.ds(me * wrows, wrows), at : at + wide], ls.at[1 + i])
        copy.start()
        own_weights.append(copy)
    with jax.named_scope("k_barrier"):
        pl.semaphore_wait(barrier, n_sp)

    def w_rows(s, h):
        return pl.ds(s * wrows + h * hrows, hrows)

    parts = {"v": (0, 1), "q": (2,)}

    def w_send(name, part):
        for dk in (0, 1):
            for i, (ref, wide, at) in enumerate(spans):
                if i in parts[part]:
                    columns = pl.ds(pl.multiple_of(unit(name, dk) * wide, 128), wide)
                    send(f"w{name}{dk}{i}", ref.at[pl.ds(half * hrows, hrows), columns], w_s.at[w_rows(me, half), at : at + wide],
                         device(name, dk))

    w_send("T", "v")
    w_send("K", "v")
    w_send("T", "q")
    for i, (ref, wide, at) in enumerate(spans):
        columns = pl.ds(pl.multiple_of(unit("S", 1) * wide, 128), wide)
        send(f"wP{i}", ref.at[:, columns], w_s.at[pl.ds(me * wrows, wrows), at : at + wide], partner)

    load_x.wait()
    step = 32

    def norm(i, _):
        here = pl.ds(k * own + i * step, step)
        wide = a_s[here, :].astype(jnp.float32)
        scale = lax.rsqrt(jnp.mean(wide * wide, -1, keepdims=True) + 1e-6)
        a_s[here, :] = (wide * scale * gain_ref[...].astype(jnp.float32)[None]).astype(jnp.bfloat16)

    with jax.named_scope("norm"):
        lax.fori_loop(0, own // step, norm, None)
    xh = own // 2
    for p in (0, 1):
        src = a_s.at[pl.ds(k * own + p * xh, xh)]
        send(f"xT{p}", src, a_s.at[pl.ds(two + k * own + p * xh, xh)], device("T"))
    send("xP", a_s.at[here_own], a_s.at[here_own], partner)

    oh = orows // 2
    tiles = depth // WIDE
    edges = [0, (tiles - tiles // 3 - tiles // 4) * WIDE, (tiles - tiles // 4) * WIDE, depth]

    def o_at(s, h, p):
        return full_ref.at[pl.ds(s * orows + h * oh, oh), edges[p] : edges[p + 1]]

    late = {}

    def o_copies(name, p, which):
        h = half if which == "half" else other
        src = wo_ref.at[pl.ds(h * oh, oh), edges[p] : edges[p + 1]]
        return [(f"{'o' if which == 'half' else 'of'}{name}{p}", src, o_at(me, h, p), device(name))]

    def fire(make, *args):
        for entry in make(*args):
            copy_of(*entry).start()
        late[(make.__name__, *args)] = (make, args)

    def o_send(name, p, which="half"):
        fire(o_copies, name, p, which)

    o_send("T", 0)
    o_send("T", 1)

    def w_block(name, dk, h, i):
        _, wide, at = spans[i]
        return w_s.at[w_rows(device(name, dk), h), at : at + wide]

    def w_on(name, dk, i):
        block = w_block(name, dk, half, i)
        recv(f"w{name}{dk}{i}", block)
        if name == "T":
            send(f"wO{dk}{i}", block, block, device("K"))
        send(f"g{name}{dk}{i}", block, block, pair)

    for dk in (0, 1):
        for i in parts["v"]:
            w_on("T", dk, i)
            w_on("K", dk, i)
    w_send("K", "q")
    for dk in (0, 1):
        for i in parts["v"]:
            w_on("O", dk, i)
    for dk in (0, 1):
        w_on("T", dk, 2)
    o_send("K", 0)
    for dk in (0, 1):
        w_on("K", dk, 2)

    def w_ready(part):
        for i in parts[part]:
            _, wide, at = spans[i]
            recv(f"wP{i}", w_s.at[pl.ds(partner * wrows, wrows), at : at + wide])
            own_weights[i].wait()
            for name in "TKO":
                for dk in (0, 1):
                    recv(f"g{name}{dk}{i}", w_block(name, dk, other, i))

    first_half = lax.broadcasted_iota(jnp.int32, (own, HEAD), 1) < HEAD // 2
    pairs = kc // (2 * HEAD)
    pw = 2 * HEAD

    def rotation(place):
        angle = (place + lax.broadcasted_iota(jnp.int32, (own, HEAD), 0)).astype(jnp.float32) * freq_ref[...]
        cos, sin = jnp.cos(angle), jnp.sin(angle)
        return cos, jnp.where(first_half, -sin, sin)

    def product(rows, at):
        return _dot(a_s[rows, :], w_s[:, pl.ds(pl.multiple_of(at, pw), pw)], 1, 0).astype(jnp.bfloat16)

    def turned(got, cos, sin):
        wide = got.astype(jnp.float32)
        heads = [wide[:, :HEAD], wide[:, HEAD:]]
        return jnp.concatenate([t * cos + pltpu.roll(t, HEAD // 2, 1) * sin for t in heads], 1).astype(jnp.bfloat16)

    def place_of(slot, core):
        return ((c if slot == 0 else mirror) * 2 + core) * own

    def project_kv(slot, core):
        rows, place = pl.ds(slot * two + core * own, own), place_of(slot, core)
        with jax.named_scope("project_kv"):
            cos, sin = rotation(place)

            def one(b, _):
                kv_s[b, pl.ds(place, own), :pw] = turned(product(rows, b * pw), cos, sin)
                kv_s[b, pl.ds(place, own), pw:] = product(rows, kc + b * pw)

            lax.fori_loop(0, pairs, one, None)

    def project_q(first, last):
        with jax.named_scope("project_q"):

            def some(i, _):
                slot, core = lax.div(i, 2), lax.rem(i, 2)
                rows = pl.ds(i * own, own)
                cos, sin = rotation((jnp.where(slot == 0, c, mirror) * 2 + core) * own)

                def one(b, _):
                    for j in (0, 1):
                        q_s[b, rows, j * pw : (j + 1) * pw] = turned(product(rows, 2 * kc + (2 * b + j) * pw), cos, sin)

                lax.fori_loop(0, pairs, one, None)

            lax.fori_loop(first, last, some, None)

    def kv_rows(chunk, b):
        return kv_s.at[b, pl.ds(chunk * two, two), :]

    def kv_send(slot):
        chunk = c if slot == 0 else mirror
        for b in range(pairs):
            send(f"kv{slot}{b}", kv_rows(chunk, b), kv_rows(chunk, b), device("K"), when=chunk < chips - 1)

    def kv_recv(b):
        recv(f"kv0{b}", kv_rows(mate, b), when=mate < chips - 1)
        recv(f"kv1{b}", kv_rows(across, b), when=across < chips - 1)

    whole_pieces = {("T", 2), ("K", 2)}

    def on_copies(name, p):
        piece = o_at(device(name), half, p)
        found = []
        if (name, p) == ("K", 0):
            found.append(("oO0", piece, piece, device("T")))
        if name == "T" and p:
            found.append((f"oO{p}", piece, piece, device("K")))
        if (name, p) not in whole_pieces:
            found.append((f"og{name}{p}", piece, piece, pair))
        return found + [(f"od{name}{p}", piece, piece, partner)]

    def over_copies(name, p):
        piece = o_at(device(name), other, p)
        return [(f"oe{name}{p}", piece, piece, partner)]

    def wo_on(name, p):
        recv(f"o{name}{p}", o_at(device(name), half, p))
        fire(on_copies, name, p)

    def wo_over(name, p):
        recv(f"of{name}{p}" if (name, p) in whole_pieces else f"og{name}{p}", o_at(device(name), other, p))
        fire(over_copies, name, p)

    w_ready("v")
    recv("xP", a_s.at[pl.ds((1 - k) * own, own)])
    project_kv(0, k)
    w_on("O", 0, 2)
    project_kv(0, 1 - k)
    w_on("O", 1, 2)
    kv_send(0)
    send("oP", wo_ref, full_ref.at[pl.ds(me * orows, orows)], partner)
    for p in (0, 1):
        got = a_s.at[pl.ds(two + k * own + p * xh, xh)]
        recv(f"xT{p}", got)
        send(f"xp{p}", got, got, partner)
        if p == 0:
            wo_on("K", 0)
            o_send("T", 2)
    project_kv(1, k)
    for p in (0, 1):
        recv(f"xp{p}", a_s.at[pl.ds(two + (1 - k) * own + p * xh, xh)])
    project_kv(1, 1 - k)
    kv_send(1)
    w_ready("q")
    project_q(0, 1)
    wo_on("T", 0)
    project_q(1, 3)
    wo_on("T", 1)
    o_send("K", 1)
    project_q(3, 4)
    sent("x", "g", "w")
    keep_wo = pltpu.make_async_copy(wo_ref, a_s.at[pl.ds(2 * own, own)], ls.at[0])
    keep_wo.start()
    load_x = pltpu.make_async_copy(x_ref, a_s.at[pl.ds(0, own)], ls.at[1])
    load_x.start()
    put_wo = pltpu.make_async_copy(a_s.at[pl.ds(2 * own, own)], full_ref.at[pl.ds(me * orows, orows)], ls.at[0])

    scale = HEAD**-0.5
    e = scale * LOG2E
    heads, share = 4, 2
    ones = jnp.ones((8, own), jnp.bfloat16)
    dv = HEAD

    def blocks_before(t):
        b, i = lax.div(t, 4), lax.rem(t, 4)
        far, near = mirror * 2 + 1, c * 2 + 1
        done = b * (2 * far + 2 * near + 2)
        done = done + jnp.where(i > 0, far + 1 - k, 0) + jnp.where(i > 1, far + k, 0)
        return done + jnp.where(i > 2, near + 1 - k, 0)

    def attend(slot, core, b, done):
        rows = pl.ds(slot * two + core * own, own)
        block_here = jnp.where(slot == 0, c, mirror) * 2 + core
        top_s[...] = jnp.full(top_s.shape, NEG, jnp.float32)
        mix_s[...] = jnp.zeros(mix_s.shape, jnp.float32)

        def block(j, masked):
            keys = pl.ds(j * own, own)
            scores = []
            for h in range(heads):
                at = (h // share) * HEAD
                scores.append(_dot(kv_s[b, keys, at : at + HEAD], q_s[b, rows, h * HEAD : (h + 1) * HEAD], 1, 1))
            if masked:
                ok = lax.broadcasted_iota(jnp.int32, (own, own), 1) >= lax.broadcasted_iota(jnp.int32, (own, own), 0)
            weights, keeps = [], []
            for h, s in enumerate(scores):
                if masked:
                    s = jnp.where(ok, s, HIDDEN)
                old = top_s[h : h + 1, :]
                top = jnp.maximum(old, s.max(axis=0, keepdims=True))
                top_s[h : h + 1, :] = top
                weights.append(jnp.exp2((s - top) * e).astype(jnp.bfloat16))
                keeps.append(jnp.exp2((old - top) * e))
            for h, (p, keep) in enumerate(zip(weights, keeps)):
                at = pw + (h // share) * HEAD
                values = jnp.concatenate([kv_s[b, keys, at : at + HEAD].T, ones], axis=0)
                mix_s[h] = mix_s[h] * keep + _dot(values, p, 1, 0)

        def whole(j, _):
            events(done + j)
            block(j, False)

        lax.fori_loop(0, block_here, whole, None)
        events(done + block_here)
        block(block_here, True)
        for h in range(heads):
            q_s[b, rows, h * HEAD : (h + 1) * HEAD] = (mix_s[h, :dv, :] * (1 / mix_s[h, dv : dv + 1, :])).T.astype(jnp.bfloat16)

    hc = heads * HEAD
    base = len(ids)
    for i in range(6):
        ids[f"seen{i}"] = base + i

    def spot(t):
        b, i = lax.div(t, 4), lax.rem(t, 4)
        slot = jnp.where(i < 2, 1, 0)
        core = lax.rem(k + lax.rem(i + 1, 2), 2)
        return slot, core, b

    def event_at(n):
        if n == 4:
            wo_over("K", 0)
            wo_over("T", 0)
            keep_wo.wait()
            put_wo.start()
        if n == 8:
            wo_on("O", 0)
        if n == 14:
            wo_over("T", 1)
        if n == 18:
            kv_recv(1)
        if n == 19:
            wo_on("T", 2)
            o_send("K", 2)
            o_send("K", 2, "other")
        if n == 24:
            wo_on("O", 1)
        if n == 25:
            wo_over("O", 0)
        if n == 35:
            wo_on("K", 1)

    def events(unit):
        for n in (4, 8, 14, 18, 19, 24, 25, 35):
            pl.when(unit == n)(functools.partial(event_at, n))

    def seen_copy(t, to, src_unit, rows, b):
        return pltpu.make_async_remote_copy(q_s.at[b, rows], seen_s.at[:, pl.ds(pl.multiple_of(src_unit * qc + b * hc, 128), hc)],
                                            ss.at[base + t], rs.at[base + t], device_id={"sp": to}, device_id_type=MESH)

    def attention(t, _):
        slot, core, b = spot(t)
        rows = pl.ds(slot * two + core * own, own)
        with jax.named_scope("attend"):
            attend(slot, core, b, blocks_before(t))

        @pl.when(lax.rem(t, 4) < 3)
        def _():
            to = jnp.where(slot == 0, c, mirror) * 2 + core
            seen_copy(t - b, to, unit_here, rows, b).start()

        @pl.when(lax.rem(t, 4) == 3)
        def _():
            own_seen(b).start()

    def own_seen(b):
        return pltpu.make_async_copy(q_s.at[b, here_own], seen_s.at[:, pl.ds(pl.multiple_of(unit_here * qc + b * hc, 128), hc)], ls.at[2 + b])

    def o_ready(p):
        for name in "KTO":
            s = device(name, 1)
            recv(f"od{name}{p}", o_at(s, half, p))
            recv(f"oe{name}{p}", o_at(s, other, p))

    slots = (qc + 2 * kc) // WIDE

    def fetch(n):
        slot = lax.rem(n, slots)
        columns = pl.ds(pl.multiple_of(slot * WIDE, 128), WIDE)
        return pltpu.make_async_copy(full_ref.at[:, pl.ds(pl.multiple_of(n * WIDE, 128), WIDE)],
                                     w_s.at[pl.ds(0, full_ref.shape[0]), columns], ls.at[4 + slot])

    def put(n):
        columns = pl.ds(pl.multiple_of(n * WIDE, 128), WIDE)
        return pltpu.make_async_copy(a_s.at[pl.ds(own, own), columns], y_ref.at[:, columns], ls.at[4 + slots + n])

    def outputs(first, last):
        def tile(n, _):
            fetch(n).wait()
            columns = pl.ds(pl.multiple_of(n * WIDE, 128), WIDE)
            slot = pl.ds(pl.multiple_of(lax.rem(n, slots) * WIDE, 128), WIDE)
            got = _dot(seen_s[...], w_s[pl.ds(0, full_ref.shape[0]), slot], 1, 0)
            a_s[pl.ds(own, own), columns] = (a_s[pl.ds(0, own), columns].astype(jnp.float32) + got).astype(jnp.bfloat16)
            put(n).start()

        with jax.named_scope("outputs"):
            lax.fori_loop(first, last, tile, None)

    def fetch_piece(p):
        lax.fori_loop(edges[p] // WIDE, edges[p + 1] // WIDE, lambda n, _: fetch(n).start(), None)

    def outputs_piece(p):
        outputs(edges[p] // WIDE, edges[p + 1] // WIDE)

    kv_recv(0)
    lax.fori_loop(0, 8, attention, None)
    o_send("T", 2, "other")
    put_wo.wait()
    recv("oP", full_ref.at[pl.ds(partner * orows, orows)])
    o_ready(0)
    fetch_piece(0)

    with jax.named_scope("finish"):
        for b in (0, 1):
            for i in range(3):
                slot = 1 if i < 2 else 0
                core = lax.rem(k + (i + 1) % 2, 2)
                to = (mirror if slot else c) * 2 + core
                seen_copy(3 * b + i, to, unit_here, pl.ds(slot * two + core * own, own), b).wait_send()
                name, dk = ("T", (i + 1) % 2) if i < 2 else ("S", 1)
                seen_copy(3 * b + i, partner, unit(name, dk), pl.ds(0, own), b).wait_recv()
            own_seen(b).wait()
        load_x.wait()

    outputs_piece(0)
    wo_on("O", 2)
    wo_over("O", 1)
    wo_over("K", 1)
    o_ready(1)
    fetch_piece(1)
    outputs_piece(1)
    wo_on("K", 2)
    wo_over("T", 2)
    wo_over("O", 2)
    wo_over("K", 2)
    o_ready(2)
    fetch_piece(2)
    outputs_piece(2)
    sent()
    for make, args in late.values():
        for entry in make(*args):
            copy_of(*entry).wait_send()
    lax.fori_loop(0, tiles, lambda n, _: put(n).wait(), None)


def solution(mesh):
    n_sp = mesh.shape["sp"]

    def step(x, gain, wq, wk, wv, wo):
        own, depth = x.shape
        units = n_sp // 2
        columns = (wq.shape[1] + wk.shape[1] + wv.shape[1]) // units
        half = HEAD // 2
        freq = THETA ** (-jnp.arange(half, dtype=jnp.float32) / half)
        freq = jnp.concatenate([freq, freq])[None]
        kc = wk.shape[1] // units
        pairs = kc // (2 * HEAD)
        hbm, vmem = pl.BlockSpec(memory_space=pltpu.HBM), pl.BlockSpec(memory_space=pltpu.VMEM)
        y, _ = pl.pallas_call(
            functools.partial(_kernel, n_sp),
            out_shape=[jax.ShapeDtypeStruct((own, depth), jnp.bfloat16),
                       jax.ShapeDtypeStruct((wo.shape[0] * n_sp, depth), jnp.bfloat16)],
            in_specs=[hbm, vmem, vmem, hbm, hbm, hbm, hbm],
            out_specs=[hbm, hbm],
            scratch_shapes=[
                pltpu.VMEM((4 * own, depth), jnp.bfloat16),
                pltpu.VMEM((wq.shape[0] * n_sp, columns), jnp.bfloat16),
                pltpu.VMEM((pairs, 4 * own, 4 * HEAD), jnp.bfloat16),
                pltpu.VMEM((pairs, own * n_sp, 4 * HEAD), jnp.bfloat16),
                pltpu.VMEM((own, wq.shape[1]), jnp.bfloat16),
                pltpu.VMEM((4, own), jnp.float32),
                pltpu.VMEM((4, HEAD + 8, own), jnp.float32),
                pltpu.SemaphoreType.DMA((112,)),
                pltpu.SemaphoreType.DMA((112,)),
                pltpu.SemaphoreType.DMA((20,)),
            ],
            compiler_params=pltpu.CompilerParams(collective_id=0, has_side_effects=True, vmem_limit_bytes=VMEM),
        )(x, gain, freq, wq, wk, wv, wo)
        return y

    tokens, whole = P(("dp", "sp"), None), P("sp", None)
    return jax.shard_map(
        step,
        mesh=mesh,
        in_specs=(tokens, P(None), whole, whole, whole, whole),
        out_specs=tokens,
        check_vma=False,
    )
```

```python
import functools

import jax
import jax.numpy as jnp
import numpy as np
from jax import lax
from jax.experimental import pallas as pl
from jax.experimental.pallas import tpu as pltpu
from jax.sharding import PartitionSpec as P

HEAD = 128
THETA = 10000
NEG = -1e30
HIDDEN = 2 * NEG
LOG2E = 1.4426950408889634
VMEM = 67043328
MESH = pl.DeviceIdType.MESH
WIDE = 256


def _dot(a, b, ca, cb):
    return lax.dot_general(a, b, (((ca,), (cb,)), ((), ())), preferred_element_type=jnp.float32)


def _kernel(n_sp, x_ref, gain_ref, freq_ref, wq_ref, wk_ref, wv_ref, wo_ref, y_ref, full_ref,
            a_s, w_s, q_s, kv_s, seen_s, top_s, mix_s, acc_s, gain_s, freq_s, ss, rs, ls):
    me, group = lax.axis_index("sp"), lax.axis_index("dp")
    chips = n_sp // 2
    c, k = lax.div(me, 2), lax.rem(me, 2)
    half = lax.rem(group, 2)
    other = 1 - half
    pair = {"dp": group + 1 - 2 * half, "sp": me}
    own, depth = x_ref.shape
    wrows = wq_ref.shape[0]
    hrows = wrows // 2
    orows = wo_ref.shape[0]
    units = chips
    qc, kc = wq_ref.shape[1] // units, wk_ref.shape[1] // units
    two = 2 * own

    mate, mirror = c + 1 - 2 * lax.rem(c, 2), chips - 1 - c
    across = chips - 1 - mate
    chip = {"S": c, "K": mate, "T": mirror, "O": across}

    def device(name, dk=0):
        return chip[name] * 2 + lax.rem(k + dk, 2)

    def unit(name, dk=0):
        return lax.div(chip[name], chips // 2) * 2 + lax.rem(k + dk, 2)

    partner = device("S", 1)
    unit_here = unit("S")

    ids = {}
    started = []

    def copy_of(name, src, dst, to):
        i = ids.setdefault(name, len(ids))
        return pltpu.make_async_remote_copy(src, dst, ss.at[i], rs.at[i], device_id=to if isinstance(to, dict) else {"sp": to},
                                            device_id_type=MESH)

    def send(name, src, dst, to, when=None):
        copy = copy_of(name, src, dst, to)
        if when is None:
            copy.start()
        else:
            pl.when(when)(copy.start)
        started.append((name, copy, when))

    def recv(name, dst, when=None):
        with jax.named_scope(f"recv_{name}"):
            copy = copy_of(name, dst, dst, partner)
            if when is None:
                copy.wait_recv()
            else:
                pl.when(when)(copy.wait_recv)

    def sent(*names):
        with jax.named_scope("sent"):
            for entry in list(started):
                name, copy, when = entry
                if not names or any(name.startswith(n) for n in names):
                    if when is None:
                        copy.wait_send()
                    else:
                        pl.when(when)(copy.wait_send)
                    started.remove(entry)

    barrier = pltpu.get_barrier_semaphore()
    for name in "SKTO":
        for dk in (0, 1):
            if (name, dk) != ("S", 0):
                pl.semaphore_signal(barrier, inc=1, device_id={"sp": device(name, dk)}, device_id_type=MESH)
    pl.semaphore_signal(barrier, inc=1, device_id=pair, device_id_type=MESH)
    here_own = pl.ds(k * own, own)
    load_x = pltpu.make_async_copy(x_ref, a_s.at[here_own], ls.at[0])
    load_x.start()
    small = [pltpu.make_async_copy(gain_ref, gain_s, ls.at[5]), pltpu.make_async_copy(freq_ref, freq_s, ls.at[6])]
    for copy in small:
        copy.start()
    spans = ((wk_ref, kc, 0), (wv_ref, kc, kc), (wq_ref, qc, 2 * kc))
    own_weights = []
    for i, (ref, wide, at) in enumerate(spans):
        copy = pltpu.make_async_copy(ref.at[:, pl.ds(pl.multiple_of(unit_here * wide, 128), wide)],
                                     w_s.at[pl.ds(me * wrows, wrows), at : at + wide], ls.at[1 + i])
        copy.start()
        own_weights.append(copy)
    with jax.named_scope("k_barrier"):
        pl.semaphore_wait(barrier, n_sp)

    def w_rows(s, h):
        return pl.ds(s * wrows + h * hrows, hrows)

    parts = {"v": (0, 1), "q": (2,)}

    def w_send(name, part):
        for dk in (0, 1):
            for i, (ref, wide, at) in enumerate(spans):
                if i in parts[part]:
                    columns = pl.ds(pl.multiple_of(unit(name, dk) * wide, 128), wide)
                    send(f"w{name}{dk}{i}", ref.at[pl.ds(half * hrows, hrows), columns], w_s.at[w_rows(me, half), at : at + wide],
                         device(name, dk))

    w_send("T", "v")
    w_send("K", "v")
    w_send("T", "q")
    for i, (ref, wide, at) in enumerate(spans):
        columns = pl.ds(pl.multiple_of(unit("S", 1) * wide, 128), wide)
        send(f"wP{i}", ref.at[:, columns], w_s.at[pl.ds(me * wrows, wrows), at : at + wide], partner)

    load_x.wait()
    for copy in small:
        copy.wait()
    step = 32

    def norm(i, _):
        here = pl.ds(k * own + i * step, step)
        wide = a_s[here, :].astype(jnp.float32)
        scale = lax.rsqrt(jnp.mean(wide * wide, -1, keepdims=True) + 1e-6)
        a_s[here, :] = (wide * scale * gain_s[...].astype(jnp.float32)[None]).astype(jnp.bfloat16)

    with jax.named_scope("norm"):
        lax.fori_loop(0, own // step, norm, None)
    xh = own // 2
    for p in (0, 1):
        src = a_s.at[pl.ds(k * own + p * xh, xh)]
        send(f"xT{p}", src, a_s.at[pl.ds(two + k * own + p * xh, xh)], device("T"))
    send("xP", a_s.at[here_own], a_s.at[here_own], partner)

    oh = orows // 2
    tiles = depth // WIDE
    edges = [n * WIDE for n in (0, tiles * 8 // 18, tiles * 13 // 18, tiles * 16 // 18, tiles)]

    def o_at(s, h, p):
        return full_ref.at[pl.ds(s * orows + h * oh, oh), edges[p] : edges[p + 1]]

    late = {}

    def o_copies(name, p, which):
        h = half if which == "half" else other
        src = wo_ref.at[pl.ds(h * oh, oh), edges[p] : edges[p + 1]]
        return [(f"{'o' if which == 'half' else 'of'}{name}{p}", src, o_at(me, h, p), device(name))]

    def fire(make, *args):
        for entry in make(*args):
            copy_of(*entry).start()
        late[(make.__name__, *args)] = (make, args)

    def o_send(name, p, which="half"):
        fire(o_copies, name, p, which)

    o_send("T", 0)
    o_send("T", 1)

    def w_block(name, dk, h, i):
        _, wide, at = spans[i]
        return w_s.at[w_rows(device(name, dk), h), at : at + wide]

    def w_on(name, dk, i):
        block = w_block(name, dk, half, i)
        recv(f"w{name}{dk}{i}", block)
        if name == "T":
            send(f"wO{dk}{i}", block, block, device("K"))
        send(f"g{name}{dk}{i}", block, block, pair)

    for dk in (0, 1):
        for i in parts["v"]:
            w_on("T", dk, i)
            w_on("K", dk, i)
    w_send("K", "q")
    for dk in (0, 1):
        for i in parts["v"]:
            w_on("O", dk, i)
    for dk in (0, 1):
        w_on("T", dk, 2)
    o_send("K", 0)
    for dk in (0, 1):
        w_on("K", dk, 2)

    def w_ready(part):
        for i in parts[part]:
            _, wide, at = spans[i]
            recv(f"wP{i}", w_s.at[pl.ds(partner * wrows, wrows), at : at + wide])
            own_weights[i].wait()
            for name in "TKO":
                for dk in (0, 1):
                    recv(f"g{name}{dk}{i}", w_block(name, dk, other, i))

    first_half = lax.broadcasted_iota(jnp.int32, (own, HEAD), 1) < HEAD // 2
    pairs = kc // (2 * HEAD)
    pw = 2 * HEAD

    def rotation(place):
        angle = (place + lax.broadcasted_iota(jnp.int32, (own, HEAD), 0)).astype(jnp.float32) * freq_s[...]
        cos, sin = jnp.cos(angle), jnp.sin(angle)
        return cos, jnp.where(first_half, -sin, sin)

    def product(rows, at):
        return _dot(a_s[rows, :], w_s[:, pl.ds(pl.multiple_of(at, pw), pw)], 1, 0).astype(jnp.bfloat16)

    def turned(got, cos, sin):
        wide = got.astype(jnp.float32)
        heads = [wide[:, :HEAD], wide[:, HEAD:]]
        return jnp.concatenate([t * cos + pltpu.roll(t, HEAD // 2, 1) * sin for t in heads], 1).astype(jnp.bfloat16)

    def place_of(slot, core):
        return ((c if slot == 0 else mirror) * 2 + core) * own

    def project_kv(slot, core):
        rows, place = pl.ds(slot * two + core * own, own), place_of(slot, core)
        with jax.named_scope("project_kv"):
            cos, sin = rotation(place)

            def one(b, _):
                kv_s[b, pl.ds(place, own), :pw] = turned(product(rows, b * pw), cos, sin)
                kv_s[b, pl.ds(place, own), pw:] = product(rows, kc + b * pw)

            lax.fori_loop(0, pairs, one, None)

    def project_q(first, last):
        with jax.named_scope("project_q"):

            def some(i, _):
                slot, core = lax.div(i, 2), lax.rem(i, 2)
                rows = pl.ds(i * own, own)
                cos, sin = rotation((jnp.where(slot == 0, c, mirror) * 2 + core) * own)

                def one(b, _):
                    for j in (0, 1):
                        q_s[b, rows, j * pw : (j + 1) * pw] = turned(product(rows, 2 * kc + (2 * b + j) * pw), cos, sin)

                lax.fori_loop(0, pairs, one, None)

            lax.fori_loop(first, last, some, None)

    def kv_rows(chunk, b):
        return kv_s.at[b, pl.ds(chunk * two, two), :]

    def kv_send(slot):
        chunk = c if slot == 0 else mirror
        for b in range(pairs):
            send(f"kv{slot}{b}", kv_rows(chunk, b), kv_rows(chunk, b), device("K"), when=chunk < chips - 1)

    def kv_recv(b):
        recv(f"kv0{b}", kv_rows(mate, b), when=mate < chips - 1)
        recv(f"kv1{b}", kv_rows(across, b), when=across < chips - 1)

    whole_pieces = {(name, p) for name in "TK" for p in (2, 3)}

    def on_copies(name, p):
        piece = o_at(device(name), half, p)
        found = []
        if (name, p) == ("K", 0):
            found.append(("oO0", piece, piece, device("T")))
        if name == "T" and p:
            found.append((f"oO{p}", piece, piece, device("K")))
        if (name, p) not in whole_pieces:
            found.append((f"og{name}{p}", piece, piece, pair))
        return found + [(f"od{name}{p}", piece, piece, partner)]

    def over_copies(name, p):
        piece = o_at(device(name), other, p)
        return [(f"oe{name}{p}", piece, piece, partner)]

    def wo_on(name, p):
        recv(f"o{name}{p}", o_at(device(name), half, p))
        fire(on_copies, name, p)

    def wo_over(name, p):
        recv(f"of{name}{p}" if (name, p) in whole_pieces else f"og{name}{p}", o_at(device(name), other, p))
        fire(over_copies, name, p)

    w_ready("v")
    recv("xP", a_s.at[pl.ds((1 - k) * own, own)])
    project_kv(0, k)
    w_on("O", 0, 2)
    project_kv(0, 1 - k)
    w_on("O", 1, 2)
    kv_send(0)
    send("oP", wo_ref, full_ref.at[pl.ds(me * orows, orows)], partner)
    for p in (0, 1):
        got = a_s.at[pl.ds(two + k * own + p * xh, xh)]
        recv(f"xT{p}", got)
        send(f"xp{p}", got, got, partner)
        if p == 0:
            wo_on("K", 0)
            o_send("T", 2)
            o_send("T", 3)
    project_kv(1, k)
    for p in (0, 1):
        recv(f"xp{p}", a_s.at[pl.ds(two + (1 - k) * own + p * xh, xh)])
    project_kv(1, 1 - k)
    kv_send(1)
    w_ready("q")
    project_q(0, 2)
    wo_on("T", 0)
    project_q(2, 4)
    sent("x", "g", "w")
    keep_wo = pltpu.make_async_copy(wo_ref, a_s.at[pl.ds(2 * own, own)], ls.at[0])
    keep_wo.start()
    load_x = pltpu.make_async_copy(x_ref, a_s.at[pl.ds(0, own)], ls.at[1])
    load_x.start()
    put_wo = pltpu.make_async_copy(a_s.at[pl.ds(2 * own, own)], full_ref.at[pl.ds(me * orows, orows)], ls.at[0])

    scale = HEAD**-0.5
    e = scale * LOG2E
    heads, share = 4, 2
    ones = jnp.ones((8, own), jnp.bfloat16)
    dv = HEAD

    def blocks_before(t):
        b, i = lax.div(t, 3), lax.rem(t, 3)
        far, near = mirror * 2 + 1, c * 2 + 1
        first, second, third, fourth = far + 1 - k, far + k, near + 1 - k, near + k
        done = b * (first + second + third) + jnp.where(i > 0, first, 0) + jnp.where(i > 1, second, 0)
        return jnp.where(t < 6, done, 2 * (first + second + third) + (t - 6) * fourth)

    def attend(slot, core, b, done):
        rows = pl.ds(slot * two + core * own, own)
        block_here = jnp.where(slot == 0, c, mirror) * 2 + core
        top_s[...] = jnp.full(top_s.shape, NEG, jnp.float32)
        mix_s[...] = jnp.zeros(mix_s.shape, jnp.float32)

        def block(j, masked):
            keys = pl.ds(j * own, own)
            scores = []
            for h in range(heads):
                at = (h // share) * HEAD
                scores.append(_dot(kv_s[b, keys, at : at + HEAD], q_s[b, rows, h * HEAD : (h + 1) * HEAD], 1, 1))
            if masked:
                ok = lax.broadcasted_iota(jnp.int32, (own, own), 1) >= lax.broadcasted_iota(jnp.int32, (own, own), 0)
            weights, keeps = [], []
            for h, s in enumerate(scores):
                if masked:
                    s = jnp.where(ok, s, HIDDEN)
                old = top_s[h : h + 1, :]
                top = jnp.maximum(old, s.max(axis=0, keepdims=True))
                top_s[h : h + 1, :] = top
                weights.append(jnp.exp2((s - top) * e).astype(jnp.bfloat16))
                keeps.append(jnp.exp2((old - top) * e))
            for h, (p, keep) in enumerate(zip(weights, keeps)):
                at = pw + (h // share) * HEAD
                values = jnp.concatenate([kv_s[b, keys, at : at + HEAD].T, ones], axis=0)
                mix_s[h] = mix_s[h] * keep + _dot(values, p, 1, 0)

        def whole(j, _):
            events(done + j)
            block(j, False)

        lax.fori_loop(0, block_here, whole, None)
        events(done + block_here)
        block(block_here, True)
        for h in range(heads):
            q_s[b, rows, h * HEAD : (h + 1) * HEAD] = (mix_s[h, :dv, :] * (1 / mix_s[h, dv : dv + 1, :])).T.astype(jnp.bfloat16)

    hc = heads * HEAD
    base = len(ids)
    for i in range(6):
        ids[f"seen{i}"] = base + i

    def spot(t):
        b = jnp.where(t < 6, lax.div(t, 3), t - 6)
        i = jnp.where(t < 6, lax.rem(t, 3), 3)
        slot = jnp.where(i < 2, 1, 0)
        core = lax.rem(k + lax.rem(i + 1, 2), 2)
        return slot, core, b

    def event_at(n):
        if n == 1:
            wo_on("T", 1)
            o_send("K", 1)
        if n == 3:
            wo_over("K", 0)
            keep_wo.wait()
            put_wo.start()
        if n == 11:
            wo_over("T", 0)
        if n == 14:
            wo_on("O", 0)
        if n == 20:
            wo_over("T", 1)
        if n == 22:
            wo_on("T", 2)
            wo_on("T", 3)
            for p in (2, 3):
                o_send("K", p)
                o_send("K", p, "other")
        if n == 25:
            wo_on("O", 1)
        if n == 33:
            wo_on("K", 1)
        if n == 35:
            wo_over("O", 0)

    def events(unit):
        for n in (1, 3, 11, 14, 20, 22, 25, 33, 35):
            pl.when(unit == n)(functools.partial(event_at, n))

    def seen_copy(t, to, src_unit, rows, b):
        return pltpu.make_async_remote_copy(q_s.at[b, rows], seen_s.at[:, pl.ds(pl.multiple_of(src_unit * qc + b * hc, 128), hc)],
                                            ss.at[base + t], rs.at[base + t], device_id={"sp": to}, device_id_type=MESH)

    def attention(t, _):
        slot, core, b = spot(t)
        rows = pl.ds(slot * two + core * own, own)
        pl.when(t == 3)(lambda: kv_recv(1))
        with jax.named_scope("attend"):
            attend(slot, core, b, blocks_before(t))

        @pl.when(t < 6)
        def _():
            to = jnp.where(slot == 0, c, mirror) * 2 + core
            seen_copy(t, to, unit_here, rows, b).start()

        @pl.when(t >= 6)
        def _():
            own_seen(b).start()

    def own_seen(b):
        return pltpu.make_async_copy(q_s.at[b, here_own], seen_s.at[:, pl.ds(pl.multiple_of(unit_here * qc + b * hc, 128), hc)], ls.at[2 + b])

    def o_ready(p):
        for name in "KTO":
            s = device(name, 1)
            recv(f"od{name}{p}", o_at(s, half, p))
            recv(f"oe{name}{p}", o_at(s, other, p))

    slots = (qc + 2 * kc) // WIDE

    def fetch(n):
        slot = lax.rem(n, slots)
        columns = pl.ds(pl.multiple_of(slot * WIDE, 128), WIDE)
        return pltpu.make_async_copy(full_ref.at[:, pl.ds(pl.multiple_of(n * WIDE, 128), WIDE)],
                                     w_s.at[pl.ds(0, full_ref.shape[0]), columns], ls.at[4 + slot])

    def put(n):
        columns = pl.ds(pl.multiple_of(n * WIDE, 128), WIDE)
        return pltpu.make_async_copy(a_s.at[pl.ds(own, own), columns], y_ref.at[:, columns], ls.at[4 + slots + n])

    def outputs(first, last):
        def tile(n, _):
            fetch(n).wait()
            columns = pl.ds(pl.multiple_of(n * WIDE, 128), WIDE)
            slot = pl.ds(pl.multiple_of(lax.rem(n, slots) * WIDE, 128), WIDE)
            got = _dot(seen_s[...], w_s[pl.ds(0, full_ref.shape[0]), slot], 1, 0)
            a_s[pl.ds(own, own), columns] = (a_s[pl.ds(0, own), columns].astype(jnp.float32) + got).astype(jnp.bfloat16)
            put(n).start()

        with jax.named_scope("outputs"):
            lax.fori_loop(first, last, tile, None)

    def fetch_piece(p):
        lax.fori_loop(edges[p] // WIDE, edges[p + 1] // WIDE, lambda n, _: fetch(n).start(), None)

    def outputs_piece(p):
        outputs(edges[p] // WIDE, edges[p + 1] // WIDE)

    kv_recv(0)
    lax.fori_loop(0, 8, attention, None)
    o_send("T", 2, "other")
    o_send("T", 3, "other")
    put_wo.wait()
    recv("oP", full_ref.at[pl.ds(partner * orows, orows)])
    o_ready(0)
    fetch_piece(0)

    near_at = lax.div(c, chips // 2) * 2 * qc
    far_at = 2 * qc - near_at
    early = acc_s.shape[1] // WIDE

    def seen_in(t):
        b, i = divmod(t, 3)
        name, dk = ("T", (i + 1) % 2) if i < 2 else ("S", 1)
        with jax.named_scope(f"seen_{t}"):
            seen_copy(t, partner, unit(name, dk), pl.ds(0, own), b).wait_recv()

    def strip(n):
        return pl.ds(pl.multiple_of(n * WIDE, 128), WIDE), pl.ds(pl.multiple_of(lax.rem(n, slots) * WIDE, 128), WIDE)

    def product_of(at, wide, slot):
        here = pl.ds(pl.multiple_of(at, 128), wide)
        return _dot(seen_s[:, here], w_s[here, slot], 1, 0)

    def early_tile(n, _):
        fetch(n).wait()
        columns, slot = strip(n)
        total = product_of(near_at, 2 * qc, slot)
        for u in (0, 1):
            total = total + product_of(far_at + u * qc, hc, slot)
        acc_s[:, columns] = total

    def late_tile(n, _):
        columns, slot = strip(n)
        total = acc_s[:, columns] + a_s[pl.ds(0, own), columns].astype(jnp.float32)
        for u in (0, 1):
            total = total + product_of(far_at + u * qc + hc, hc, slot)
        a_s[pl.ds(own, own), columns] = total.astype(jnp.bfloat16)
        put(n).start()

    for t in (0, 1, 2, 5):
        seen_in(t)
    for b in (0, 1):
        own_seen(b).wait()
    load_x.wait()
    with jax.named_scope("outputs_early"):
        lax.fori_loop(0, early, early_tile, None)
    wo_over("O", 1)
    wo_on("O", 2)
    wo_on("O", 3)
    for t in (3, 4):
        seen_in(t)
    with jax.named_scope("outputs_late"):
        lax.fori_loop(0, early, late_tile, None)
    outputs(early, edges[1] // WIDE)
    wo_on("K", 2)
    wo_over("K", 1)
    wo_over("K", 2)
    o_ready(1)
    fetch_piece(1)
    wo_on("K", 3)
    wo_over("T", 2)
    outputs_piece(1)
    wo_over("O", 2)
    wo_over("K", 3)
    wo_over("T", 3)
    wo_over("O", 3)
    for p in (2, 3):
        o_ready(p)
        fetch_piece(p)
    for p in (2, 3):
        outputs_piece(p)
    for b in (0, 1):
        for i in range(3):
            slot = 1 if i < 2 else 0
            core = lax.rem(k + (i + 1) % 2, 2)
            to = (mirror if slot else c) * 2 + core
            seen_copy(3 * b + i, to, unit_here, pl.ds(slot * two + core * own, own), b).wait_send()
    sent()
    for make, args in late.values():
        for entry in make(*args):
            copy_of(*entry).wait_send()
    lax.fori_loop(0, tiles, lambda n, _: put(n).wait(), None)


def solution(mesh):
    n_sp = mesh.shape["sp"]

    def step(x, gain, wq, wk, wv, wo):
        own, depth = x.shape
        units = n_sp // 2
        columns = (wq.shape[1] + wk.shape[1] + wv.shape[1]) // units
        half = HEAD // 2
        freq = np.float32(THETA) ** (-np.arange(half, dtype=np.float32) / half)
        freq = jnp.asarray(np.concatenate([freq, freq])[None])
        kc = wk.shape[1] // units
        pairs = kc // (2 * HEAD)
        hbm = pl.BlockSpec(memory_space=pltpu.HBM)
        y, _ = pl.pallas_call(
            functools.partial(_kernel, n_sp),
            out_shape=[jax.ShapeDtypeStruct((own, depth), jnp.bfloat16),
                       jax.ShapeDtypeStruct((wo.shape[0] * n_sp, depth), jnp.bfloat16)],
            in_specs=[hbm] * 7,
            out_specs=[hbm, hbm],
            scratch_shapes=[
                pltpu.VMEM((4 * own, depth), jnp.bfloat16),
                pltpu.VMEM((wq.shape[0] * n_sp, columns), jnp.bfloat16),
                pltpu.VMEM((pairs, 4 * own, 4 * HEAD), jnp.bfloat16),
                pltpu.VMEM((pairs, own * n_sp, 4 * HEAD), jnp.bfloat16),
                pltpu.VMEM((own, wq.shape[1]), jnp.bfloat16),
                pltpu.VMEM((4, own), jnp.float32),
                pltpu.VMEM((4, HEAD + 8, own), jnp.float32),
                pltpu.VMEM((own, depth // 3), jnp.float32),
                pltpu.VMEM(gain.shape, jnp.bfloat16),
                pltpu.VMEM(freq.shape, jnp.float32),
                pltpu.SemaphoreType.DMA((112,)),
                pltpu.SemaphoreType.DMA((112,)),
                pltpu.SemaphoreType.DMA((32,)),
            ],
            compiler_params=pltpu.CompilerParams(collective_id=0, has_side_effects=True, vmem_limit_bytes=VMEM),
        )(x, gain, freq, wq, wk, wv, wo)
        return y

    tokens, whole = P(("dp", "sp"), None), P("sp", None)
    return jax.shard_map(
        step,
        mesh=mesh,
        in_specs=(tokens, P(None), whole, whole, whole, whole),
        out_specs=tokens,
        check_vma=False,
    )
```

```python
import functools

import jax
import jax.numpy as jnp
import numpy as np
from jax import lax
from jax.experimental import pallas as pl
from jax.experimental.pallas import tpu as pltpu
from jax.sharding import PartitionSpec as P

HEAD = 128
THETA = 10000
NEG = -1e30
HIDDEN = 2 * NEG
LOG2E = 1.4426950408889634
VMEM = 67043328
MESH = pl.DeviceIdType.MESH
WIDE = 256


def _dot(a, b, ca, cb):
    return lax.dot_general(a, b, (((ca,), (cb,)), ((), ())), preferred_element_type=jnp.float32)


def _kernel(n_sp, x_ref, gain_ref, freq_ref, wq_ref, wk_ref, wv_ref, wo_ref, y_ref, full_ref,
            a_s, w_s, q_s, kv_s, seen_s, top_s, mix_s, acc_s, gain_s, freq_s, ss, rs, ls):
    me, group = lax.axis_index("sp"), lax.axis_index("dp")
    chips = n_sp // 2
    c, k = lax.div(me, 2), lax.rem(me, 2)
    half = lax.rem(group, 2)
    other = 1 - half
    pair = {"dp": group + 1 - 2 * half, "sp": me}
    own, depth = x_ref.shape
    wrows = wq_ref.shape[0]
    hrows = wrows // 2
    orows = wo_ref.shape[0]
    units = chips
    qc, kc = wq_ref.shape[1] // units, wk_ref.shape[1] // units
    two = 2 * own

    mate, mirror = c + 1 - 2 * lax.rem(c, 2), chips - 1 - c
    across = chips - 1 - mate
    chip = {"S": c, "K": mate, "T": mirror, "O": across}

    def device(name, dk=0):
        return chip[name] * 2 + lax.rem(k + dk, 2)

    def unit(name, dk=0):
        return lax.div(chip[name], chips // 2) * 2 + lax.rem(k + dk, 2)

    partner = device("S", 1)
    unit_here = unit("S")

    ids = {}
    started = []

    def copy_of(name, src, dst, to):
        i = ids.setdefault(name, len(ids))
        return pltpu.make_async_remote_copy(src, dst, ss.at[i], rs.at[i], device_id=to if isinstance(to, dict) else {"sp": to},
                                            device_id_type=MESH)

    def send(name, src, dst, to, when=None):
        copy = copy_of(name, src, dst, to)
        if when is None:
            copy.start()
        else:
            pl.when(when)(copy.start)
        started.append((name, copy, when))

    def recv(name, dst, when=None):
        with jax.named_scope(f"recv_{name}"):
            copy = copy_of(name, dst, dst, partner)
            if when is None:
                copy.wait_recv()
            else:
                pl.when(when)(copy.wait_recv)

    def sent(*names):
        with jax.named_scope("sent"):
            for entry in list(started):
                name, copy, when = entry
                if not names or any(name.startswith(n) for n in names):
                    if when is None:
                        copy.wait_send()
                    else:
                        pl.when(when)(copy.wait_send)
                    started.remove(entry)

    barrier = pltpu.get_barrier_semaphore()
    for name in "SKTO":
        for dk in (0, 1):
            if (name, dk) != ("S", 0):
                pl.semaphore_signal(barrier, inc=1, device_id={"sp": device(name, dk)}, device_id_type=MESH)
    pl.semaphore_signal(barrier, inc=1, device_id=pair, device_id_type=MESH)
    here_own = pl.ds(k * own, own)
    load_x = pltpu.make_async_copy(x_ref, a_s.at[here_own], ls.at[0])
    load_x.start()
    small = [pltpu.make_async_copy(gain_ref, gain_s, ls.at[5]), pltpu.make_async_copy(freq_ref, freq_s, ls.at[6])]
    for copy in small:
        copy.start()
    spans = ((wk_ref, kc, 0), (wv_ref, kc, kc), (wq_ref, qc, 2 * kc))
    own_weights = []
    for i, (ref, wide, at) in enumerate(spans):
        copy = pltpu.make_async_copy(ref.at[:, pl.ds(pl.multiple_of(unit_here * wide, 128), wide)],
                                     w_s.at[pl.ds(me * wrows, wrows), at : at + wide], ls.at[1 + i])
        copy.start()
        own_weights.append(copy)
    with jax.named_scope("k_barrier"):
        pl.semaphore_wait(barrier, n_sp)

    def w_rows(s, h):
        return pl.ds(s * wrows + h * hrows, hrows)

    parts = {"v": (0, 1), "q": (2,)}

    def w_send(name, part):
        for dk in (0, 1):
            for i, (ref, wide, at) in enumerate(spans):
                if i in parts[part]:
                    columns = pl.ds(pl.multiple_of(unit(name, dk) * wide, 128), wide)
                    send(f"w{name}{dk}{i}", ref.at[pl.ds(half * hrows, hrows), columns], w_s.at[w_rows(me, half), at : at + wide],
                         device(name, dk))

    w_send("T", "v")
    w_send("K", "v")
    w_send("T", "q")
    for i, (ref, wide, at) in enumerate(spans):
        columns = pl.ds(pl.multiple_of(unit("S", 1) * wide, 128), wide)
        send(f"wP{i}", ref.at[:, columns], w_s.at[pl.ds(me * wrows, wrows), at : at + wide], partner)

    load_x.wait()
    for copy in small:
        copy.wait()
    step = 32

    def norm(i, _):
        here = pl.ds(k * own + i * step, step)
        wide = a_s[here, :].astype(jnp.float32)
        scale = lax.rsqrt(jnp.mean(wide * wide, -1, keepdims=True) + 1e-6)
        a_s[here, :] = (wide * scale * gain_s[...].astype(jnp.float32)[None]).astype(jnp.bfloat16)

    with jax.named_scope("norm"):
        lax.fori_loop(0, own // step, norm, None)
    xh = own // 2
    for p in (0, 1):
        src = a_s.at[pl.ds(k * own + p * xh, xh)]
        send(f"xT{p}", src, a_s.at[pl.ds(two + k * own + p * xh, xh)], device("T"))
    send("xP", a_s.at[here_own], a_s.at[here_own], partner)

    oh = orows // 2
    tiles = depth // WIDE
    edges = [n * WIDE for n in (0, tiles * 8 // 18, tiles * 13 // 18, tiles * 16 // 18, tiles)]

    def o_at(s, h, p):
        return full_ref.at[pl.ds(s * orows + h * oh, oh), edges[p] : edges[p + 1]]

    late = {}

    def o_copies(name, p, which):
        h = half if which == "half" else other
        src = wo_ref.at[pl.ds(h * oh, oh), edges[p] : edges[p + 1]]
        return [(f"{'o' if which == 'half' else 'of'}{name}{p}", src, o_at(me, h, p), device(name))]

    def fire(make, *args):
        for entry in make(*args):
            copy_of(*entry).start()
        late[(make.__name__, *args)] = (make, args)

    def o_send(name, p, which="half"):
        fire(o_copies, name, p, which)

    o_send("T", 0)
    o_send("T", 1)

    def w_block(name, dk, h, i):
        _, wide, at = spans[i]
        return w_s.at[w_rows(device(name, dk), h), at : at + wide]

    def w_on(name, dk, i):
        block = w_block(name, dk, half, i)
        recv(f"w{name}{dk}{i}", block)
        if name == "T":
            send(f"wO{dk}{i}", block, block, device("K"))
        send(f"g{name}{dk}{i}", block, block, pair)

    for dk in (0, 1):
        for i in parts["v"]:
            w_on("T", dk, i)
            w_on("K", dk, i)
    w_send("K", "q")
    for dk in (0, 1):
        for i in parts["v"]:
            w_on("O", dk, i)
    for dk in (0, 1):
        w_on("T", dk, 2)
    o_send("K", 0)
    for dk in (0, 1):
        w_on("K", dk, 2)

    def w_ready(part):
        for i in parts[part]:
            _, wide, at = spans[i]
            recv(f"wP{i}", w_s.at[pl.ds(partner * wrows, wrows), at : at + wide])
            own_weights[i].wait()
            for name in "TKO":
                for dk in (0, 1):
                    recv(f"g{name}{dk}{i}", w_block(name, dk, other, i))

    first_half = lax.broadcasted_iota(jnp.int32, (own, HEAD), 1) < HEAD // 2
    pairs = kc // (2 * HEAD)
    pw = 2 * HEAD

    def rotation(place):
        angle = (place + lax.broadcasted_iota(jnp.int32, (own, HEAD), 0)).astype(jnp.float32) * freq_s[...]
        cos, sin = jnp.cos(angle), jnp.sin(angle)
        return cos, jnp.where(first_half, -sin, sin)

    def product(rows, at):
        return _dot(a_s[rows, :], w_s[:, pl.ds(pl.multiple_of(at, pw), pw)], 1, 0).astype(jnp.bfloat16)

    def turned(got, cos, sin):
        wide = got.astype(jnp.float32)
        heads = [wide[:, :HEAD], wide[:, HEAD:]]
        return jnp.concatenate([t * cos + pltpu.roll(t, HEAD // 2, 1) * sin for t in heads], 1).astype(jnp.bfloat16)

    def place_of(slot, core):
        return ((c if slot == 0 else mirror) * 2 + core) * own

    def project_kv(slot, core):
        rows, place = pl.ds(slot * two + core * own, own), place_of(slot, core)
        with jax.named_scope("project_kv"):
            cos, sin = rotation(place)

            def one(b, _):
                kv_s[b, pl.ds(place, own), :pw] = turned(product(rows, b * pw), cos, sin)
                kv_s[b, pl.ds(place, own), pw:] = product(rows, kc + b * pw)

            lax.fori_loop(0, pairs, one, None)

    def project_q(first, last):
        with jax.named_scope("project_q"):

            def some(i, _):
                slot, core = lax.div(i, 2), lax.rem(i, 2)
                rows = pl.ds(i * own, own)
                cos, sin = rotation((jnp.where(slot == 0, c, mirror) * 2 + core) * own)

                def one(b, _):
                    for j in (0, 1):
                        q_s[b, rows, j * pw : (j + 1) * pw] = turned(product(rows, 2 * kc + (2 * b + j) * pw), cos, sin)

                lax.fori_loop(0, pairs, one, None)

            lax.fori_loop(first, last, some, None)

    def kv_rows(chunk, b):
        return kv_s.at[b, pl.ds(chunk * two, two), :]

    def kv_send(slot):
        chunk = c if slot == 0 else mirror
        for b in range(pairs):
            send(f"kv{slot}{b}", kv_rows(chunk, b), kv_rows(chunk, b), device("K"), when=chunk < chips - 1)

    def kv_recv(b):
        recv(f"kv0{b}", kv_rows(mate, b), when=mate < chips - 1)
        recv(f"kv1{b}", kv_rows(across, b), when=across < chips - 1)

    whole_pieces = {(name, p) for name in "TK" for p in (2, 3)}

    def on_copies(name, p):
        piece = o_at(device(name), half, p)
        found = []
        if (name, p) == ("K", 0):
            found.append(("oO0", piece, piece, device("T")))
        if name == "T" and p:
            found.append((f"oO{p}", piece, piece, device("K")))
        if (name, p) not in whole_pieces:
            found.append((f"og{name}{p}", piece, piece, pair))
        return found + [(f"od{name}{p}", piece, piece, partner)]

    def over_copies(name, p):
        piece = o_at(device(name), other, p)
        return [(f"oe{name}{p}", piece, piece, partner)]

    def wo_on(name, p):
        recv(f"o{name}{p}", o_at(device(name), half, p))
        fire(on_copies, name, p)

    def wo_over(name, p):
        recv(f"of{name}{p}" if (name, p) in whole_pieces else f"og{name}{p}", o_at(device(name), other, p))
        fire(over_copies, name, p)

    w_ready("v")
    recv("xP", a_s.at[pl.ds((1 - k) * own, own)])
    project_kv(0, k)
    w_on("O", 0, 2)
    project_kv(0, 1 - k)
    w_on("O", 1, 2)
    kv_send(0)
    send("oP", wo_ref, full_ref.at[pl.ds(me * orows, orows)], partner)
    for p in (0, 1):
        got = a_s.at[pl.ds(two + k * own + p * xh, xh)]
        recv(f"xT{p}", got)
        send(f"xp{p}", got, got, partner)
        if p == 0:
            wo_on("K", 0)
            o_send("T", 2)
            o_send("T", 3)
    project_kv(1, k)
    for p in (0, 1):
        recv(f"xp{p}", a_s.at[pl.ds(two + (1 - k) * own + p * xh, xh)])
    project_kv(1, 1 - k)
    kv_send(1)
    w_ready("q")
    project_q(0, 2)
    wo_on("T", 0)
    project_q(2, 4)
    sent("x", "g", "w")
    keep_wo = pltpu.make_async_copy(wo_ref, a_s.at[pl.ds(2 * own, own)], ls.at[0])
    keep_wo.start()
    load_x = pltpu.make_async_copy(x_ref, a_s.at[pl.ds(0, own)], ls.at[1])
    load_x.start()
    put_wo = pltpu.make_async_copy(a_s.at[pl.ds(2 * own, own)], full_ref.at[pl.ds(me * orows, orows)], ls.at[0])

    scale = HEAD**-0.5
    e = scale * LOG2E
    heads, share = 4, 2
    ones = jnp.ones((8, own), jnp.bfloat16)
    dv = HEAD

    def blocks_before(t):
        b, i = lax.div(t, 3), lax.rem(t, 3)
        far, near = mirror * 2 + 1, c * 2 + 1
        first, second, third, fourth = far + 1 - k, far + k, near + 1 - k, near + k
        done = b * (first + second + third) + jnp.where(i > 0, first, 0) + jnp.where(i > 1, second, 0)
        return jnp.where(t < 6, done, 2 * (first + second + third) + (t - 6) * fourth)

    def attend(slot, core, b, done):
        rows = pl.ds(slot * two + core * own, own)
        block_here = jnp.where(slot == 0, c, mirror) * 2 + core
        top_s[...] = jnp.full(top_s.shape, NEG, jnp.float32)
        mix_s[...] = jnp.zeros(mix_s.shape, jnp.float32)

        def block(j, masked):
            keys = pl.ds(j * own, own)
            scores = []
            for h in range(heads):
                at = (h // share) * HEAD
                scores.append(_dot(kv_s[b, keys, at : at + HEAD], q_s[b, rows, h * HEAD : (h + 1) * HEAD], 1, 1))
            if masked:
                ok = lax.broadcasted_iota(jnp.int32, (own, own), 1) >= lax.broadcasted_iota(jnp.int32, (own, own), 0)
            weights, keeps = [], []
            for h, s in enumerate(scores):
                if masked:
                    s = jnp.where(ok, s, HIDDEN)
                old = top_s[h : h + 1, :]
                top = jnp.maximum(old, s.max(axis=0, keepdims=True))
                top_s[h : h + 1, :] = top
                weights.append(jnp.exp2((s - top) * e).astype(jnp.bfloat16))
                keeps.append(jnp.exp2((old - top) * e))
            for h, (p, keep) in enumerate(zip(weights, keeps)):
                at = pw + (h // share) * HEAD
                values = jnp.concatenate([kv_s[b, keys, at : at + HEAD].T, ones], axis=0)
                mix_s[h] = mix_s[h] * keep + _dot(values, p, 1, 0)

        def whole(j, _):
            events(done + j)
            block(j, False)

        lax.fori_loop(0, block_here, whole, None)
        events(done + block_here)
        block(block_here, True)
        for h in range(heads):
            q_s[b, rows, h * HEAD : (h + 1) * HEAD] = (mix_s[h, :dv, :] * (1 / mix_s[h, dv : dv + 1, :])).T.astype(jnp.bfloat16)

    hc = heads * HEAD
    base = len(ids)
    for i in range(6):
        ids[f"seen{i}"] = base + i

    def spot(t):
        b = jnp.where(t < 6, lax.div(t, 3), t - 6)
        i = jnp.where(t < 6, lax.rem(t, 3), 3)
        slot = jnp.where(i < 2, 1, 0)
        core = lax.rem(k + lax.rem(i + 1, 2), 2)
        return slot, core, b

    def event_at(n):
        if n == 1:
            wo_on("T", 1)
            o_send("K", 1)
        if n == 3:
            wo_over("K", 0)
            keep_wo.wait()
            put_wo.start()
        if n == 11:
            wo_over("T", 0)
        if n == 14:
            wo_on("O", 0)
        if n == 20:
            wo_over("T", 1)
        if n == 22:
            wo_on("T", 2)
            wo_on("T", 3)
            for p in (2, 3):
                o_send("K", p)
                o_send("K", p, "other")
        if n == 25:
            wo_on("O", 1)
        if n == 33:
            wo_on("K", 1)
        if n == 35:
            wo_over("O", 0)

    def events(unit):
        for n in (1, 3, 11, 14, 20, 22, 25, 33, 35):
            pl.when(unit == n)(functools.partial(event_at, n))

    def seen_copy(t, to, src_unit, rows, b):
        return pltpu.make_async_remote_copy(q_s.at[b, rows], seen_s.at[:, pl.ds(pl.multiple_of(src_unit * qc + b * hc, 128), hc)],
                                            ss.at[base + t], rs.at[base + t], device_id={"sp": to}, device_id_type=MESH)

    def attention(t, _):
        slot, core, b = spot(t)
        rows = pl.ds(slot * two + core * own, own)
        pl.when(t == 3)(lambda: kv_recv(1))
        with jax.named_scope("attend"):
            attend(slot, core, b, blocks_before(t))

        @pl.when(t < 6)
        def _():
            to = jnp.where(slot == 0, c, mirror) * 2 + core
            seen_copy(t, to, unit_here, rows, b).start()

        @pl.when(t >= 6)
        def _():
            own_seen(b).start()

    def own_seen(b):
        return pltpu.make_async_copy(q_s.at[b, here_own], seen_s.at[:, pl.ds(pl.multiple_of(unit_here * qc + b * hc, 128), hc)], ls.at[2 + b])

    def o_ready(p):
        for name in "KTO":
            s = device(name, 1)
            recv(f"od{name}{p}", o_at(s, half, p))
            recv(f"oe{name}{p}", o_at(s, other, p))

    slots = (qc + 2 * kc) // WIDE

    def fetch(n):
        slot = lax.rem(n, slots)
        columns = pl.ds(pl.multiple_of(slot * WIDE, 128), WIDE)
        return pltpu.make_async_copy(full_ref.at[:, pl.ds(pl.multiple_of(n * WIDE, 128), WIDE)],
                                     w_s.at[pl.ds(0, full_ref.shape[0]), columns], ls.at[4 + slot])

    def put(n):
        columns = pl.ds(pl.multiple_of(n * WIDE, 128), WIDE)
        return pltpu.make_async_copy(a_s.at[pl.ds(own, own), columns], y_ref.at[:, columns], ls.at[4 + slots + n])

    def before_tile(at):
        first, second, third = (edges[p] // WIDE for p in (1, 2, 3))
        if at == first:
            wo_on("K", 2)
            wo_over("K", 1)
            wo_over("K", 2)
            o_ready(1)
            fetch_piece(1)
        if at == first + 3:
            wo_over("T", 2)
            wo_over("O", 2)
            wo_on("K", 3)
        if at == first + 4:
            o_ready(2)
            fetch_piece(2)
        if at == second:
            wo_over("K", 3)
            wo_over("T", 3)
            wo_over("O", 3)
        if at == third - 1:
            o_ready(3)
            fetch_piece(3)

    def outputs(first, last):
        def tile(n, _):
            start = edges[1] // WIDE
            for at in (start, start + 3, start + 4, edges[2] // WIDE, edges[3] // WIDE - 1):
                pl.when(n == at)(functools.partial(before_tile, at))
            fetch(n).wait()
            columns = pl.ds(pl.multiple_of(n * WIDE, 128), WIDE)
            slot = pl.ds(pl.multiple_of(lax.rem(n, slots) * WIDE, 128), WIDE)
            got = _dot(seen_s[...], w_s[pl.ds(0, full_ref.shape[0]), slot], 1, 0)
            a_s[pl.ds(own, own), columns] = (a_s[pl.ds(0, own), columns].astype(jnp.float32) + got).astype(jnp.bfloat16)
            put(n).start()

        with jax.named_scope("outputs"):
            lax.fori_loop(first, last, tile, None)

    def fetch_piece(p):
        lax.fori_loop(edges[p] // WIDE, edges[p + 1] // WIDE, lambda n, _: fetch(n).start(), None)

    kv_recv(0)
    lax.fori_loop(0, 8, attention, None)
    o_send("T", 2, "other")
    o_send("T", 3, "other")
    put_wo.wait()
    recv("oP", full_ref.at[pl.ds(partner * orows, orows)])
    o_ready(0)
    fetch_piece(0)

    near_at = lax.div(c, chips // 2) * 2 * qc
    far_at = 2 * qc - near_at
    early = acc_s.shape[1] // WIDE

    def seen_in(t):
        b, i = divmod(t, 3)
        name, dk = ("T", (i + 1) % 2) if i < 2 else ("S", 1)
        with jax.named_scope(f"seen_{t}"):
            seen_copy(t, partner, unit(name, dk), pl.ds(0, own), b).wait_recv()

    def strip(n):
        return pl.ds(pl.multiple_of(n * WIDE, 128), WIDE), pl.ds(pl.multiple_of(lax.rem(n, slots) * WIDE, 128), WIDE)

    def product_of(at, wide, slot):
        here = pl.ds(pl.multiple_of(at, 128), wide)
        return _dot(seen_s[:, here], w_s[here, slot], 1, 0)

    def early_tile(n, _):
        fetch(n).wait()
        columns, slot = strip(n)
        total = product_of(near_at, 2 * qc, slot)
        for u in (0, 1):
            total = total + product_of(far_at + u * qc, hc, slot)
        acc_s[:, columns] = total

    def late_tile(n, _):
        columns, slot = strip(n)
        total = acc_s[:, columns] + a_s[pl.ds(0, own), columns].astype(jnp.float32)
        for u in (0, 1):
            total = total + product_of(far_at + u * qc + hc, hc, slot)
        a_s[pl.ds(own, own), columns] = total.astype(jnp.bfloat16)
        put(n).start()

    for t in (0, 1, 2, 5):
        seen_in(t)
    for b in (0, 1):
        own_seen(b).wait()
    load_x.wait()
    with jax.named_scope("outputs_early"):
        lax.fori_loop(0, early, early_tile, None)
    wo_over("O", 1)
    wo_on("O", 2)
    wo_on("O", 3)
    for t in (3, 4):
        seen_in(t)
    with jax.named_scope("outputs_late"):
        lax.fori_loop(0, early, late_tile, None)
    outputs(early, tiles)
    for b in (0, 1):
        for i in range(3):
            slot = 1 if i < 2 else 0
            core = lax.rem(k + (i + 1) % 2, 2)
            to = (mirror if slot else c) * 2 + core
            seen_copy(3 * b + i, to, unit_here, pl.ds(slot * two + core * own, own), b).wait_send()
    sent()
    for make, args in late.values():
        for entry in make(*args):
            copy_of(*entry).wait_send()
    lax.fori_loop(0, tiles, lambda n, _: put(n).wait(), None)


def solution(mesh):
    n_sp = mesh.shape["sp"]

    def step(x, gain, wq, wk, wv, wo):
        own, depth = x.shape
        units = n_sp // 2
        columns = (wq.shape[1] + wk.shape[1] + wv.shape[1]) // units
        half = HEAD // 2
        freq = np.float32(THETA) ** (-np.arange(half, dtype=np.float32) / half)
        freq = jnp.asarray(np.concatenate([freq, freq])[None])
        kc = wk.shape[1] // units
        pairs = kc // (2 * HEAD)
        hbm = pl.BlockSpec(memory_space=pltpu.HBM)
        y, _ = pl.pallas_call(
            functools.partial(_kernel, n_sp),
            out_shape=[jax.ShapeDtypeStruct((own, depth), jnp.bfloat16),
                       jax.ShapeDtypeStruct((wo.shape[0] * n_sp, depth), jnp.bfloat16)],
            in_specs=[hbm] * 7,
            out_specs=[hbm, hbm],
            scratch_shapes=[
                pltpu.VMEM((4 * own, depth), jnp.bfloat16),
                pltpu.VMEM((wq.shape[0] * n_sp, columns), jnp.bfloat16),
                pltpu.VMEM((pairs, 4 * own, 4 * HEAD), jnp.bfloat16),
                pltpu.VMEM((pairs, own * n_sp, 4 * HEAD), jnp.bfloat16),
                pltpu.VMEM((own, wq.shape[1]), jnp.bfloat16),
                pltpu.VMEM((4, own), jnp.float32),
                pltpu.VMEM((4, HEAD + 8, own), jnp.float32),
                pltpu.VMEM((own, depth // 3), jnp.float32),
                pltpu.VMEM(gain.shape, jnp.bfloat16),
                pltpu.VMEM(freq.shape, jnp.float32),
                pltpu.SemaphoreType.DMA((112,)),
                pltpu.SemaphoreType.DMA((112,)),
                pltpu.SemaphoreType.DMA((32,)),
            ],
            compiler_params=pltpu.CompilerParams(collective_id=0, has_side_effects=True, vmem_limit_bytes=VMEM),
        )(x, gain, freq, wq, wk, wv, wo)
        return y

    tokens, whole = P(("dp", "sp"), None), P("sp", None)
    return jax.shard_map(
        step,
        mesh=mesh,
        in_specs=(tokens, P(None), whole, whole, whole, whole),
        out_specs=tokens,
        check_vma=False,
    )
```

```python
import functools

import jax
import jax.numpy as jnp
import numpy as np
from jax import lax
from jax.experimental import pallas as pl
from jax.experimental.pallas import tpu as pltpu
from jax.sharding import PartitionSpec as P

HEAD = 128
THETA = 10000
NEG = -1e30
HIDDEN = 2 * NEG
LOG2E = 1.4426950408889634
VMEM = 67043328
MESH = pl.DeviceIdType.MESH
WIDE = 256


def _dot(a, b, ca, cb):
    return lax.dot_general(a, b, (((ca,), (cb,)), ((), ())), preferred_element_type=jnp.float32)


def _kernel(n_sp, x_ref, gain_ref, freq_ref, wq_ref, wk_ref, wv_ref, wo_ref, y_ref, full_ref,
            a_s, w_s, q_s, kv_s, seen_s, top_s, mix_s, acc_s, gain_s, freq_s, ss, rs, ls):
    me, group = lax.axis_index("sp"), lax.axis_index("dp")
    chips = n_sp // 2
    c, k = lax.div(me, 2), lax.rem(me, 2)
    half = lax.rem(group, 2)
    other = 1 - half
    pair = {"dp": group + 1 - 2 * half, "sp": me}
    own, depth = x_ref.shape
    wrows = wq_ref.shape[0]
    hrows = wrows // 2
    orows = wo_ref.shape[0]
    units = chips
    qc, kc = wq_ref.shape[1] // units, wk_ref.shape[1] // units
    two = 2 * own

    mate, mirror = c + 1 - 2 * lax.rem(c, 2), chips - 1 - c
    across = chips - 1 - mate
    chip = {"S": c, "K": mate, "T": mirror, "O": across}

    def device(name, dk=0):
        return chip[name] * 2 + lax.rem(k + dk, 2)

    def unit(name, dk=0):
        return lax.div(chip[name], chips // 2) * 2 + lax.rem(k + dk, 2)

    partner = device("S", 1)
    unit_here = unit("S")

    ids = {}
    started = []

    def copy_of(name, src, dst, to):
        i = ids.setdefault(name, len(ids))
        return pltpu.make_async_remote_copy(src, dst, ss.at[i], rs.at[i], device_id=to if isinstance(to, dict) else {"sp": to},
                                            device_id_type=MESH)

    def send(name, src, dst, to, when=None):
        copy = copy_of(name, src, dst, to)
        if when is None:
            copy.start()
        else:
            pl.when(when)(copy.start)
        started.append((name, copy, when))

    def recv(name, dst, when=None):
        with jax.named_scope(f"recv_{name}"):
            copy = copy_of(name, dst, dst, partner)
            if when is None:
                copy.wait_recv()
            else:
                pl.when(when)(copy.wait_recv)

    def sent(*names):
        with jax.named_scope("sent"):
            for entry in list(started):
                name, copy, when = entry
                if not names or any(name.startswith(n) for n in names):
                    if when is None:
                        copy.wait_send()
                    else:
                        pl.when(when)(copy.wait_send)
                    started.remove(entry)

    barrier = pltpu.get_barrier_semaphore()
    for name in "SKT":
        for dk in (0, 1):
            if (name, dk) != ("S", 0):
                pl.semaphore_signal(barrier, inc=1, device_id={"sp": device(name, dk)}, device_id_type=MESH)
    pl.semaphore_signal(barrier, inc=1, device_id=pair, device_id_type=MESH)
    here_own = pl.ds(k * own, own)
    load_x = pltpu.make_async_copy(x_ref, a_s.at[here_own], ls.at[0])
    load_x.start()
    small = [pltpu.make_async_copy(gain_ref, gain_s, ls.at[5]), pltpu.make_async_copy(freq_ref, freq_s, ls.at[6])]
    for copy in small:
        copy.start()
    spans = ((wk_ref, kc, 0), (wv_ref, kc, kc), (wq_ref, qc, 2 * kc))
    own_weights = []
    for i, (ref, wide, at) in enumerate(spans):
        copy = pltpu.make_async_copy(ref.at[:, pl.ds(pl.multiple_of(unit_here * wide, 128), wide)],
                                     w_s.at[pl.ds(me * wrows, wrows), at : at + wide], ls.at[1 + i])
        copy.start()
        own_weights.append(copy)
    with jax.named_scope("k_barrier"):
        pl.semaphore_wait(barrier, 6)

    def w_rows(s, h):
        return pl.ds(s * wrows + h * hrows, hrows)

    parts = {"v": (0, 1), "q": (2,)}

    def w_send(name, part):
        for dk in (0, 1):
            for i, (ref, wide, at) in enumerate(spans):
                if i in parts[part]:
                    columns = pl.ds(pl.multiple_of(unit(name, dk) * wide, 128), wide)
                    send(f"w{name}{dk}{i}", ref.at[pl.ds(half * hrows, hrows), columns], w_s.at[w_rows(me, half), at : at + wide],
                         device(name, dk))

    w_send("T", "v")
    w_send("K", "v")
    w_send("T", "q")
    for i, (ref, wide, at) in enumerate(spans):
        columns = pl.ds(pl.multiple_of(unit("S", 1) * wide, 128), wide)
        send(f"wP{i}", ref.at[:, columns], w_s.at[pl.ds(me * wrows, wrows), at : at + wide], partner)

    load_x.wait()
    for copy in small:
        copy.wait()
    step = 32

    def norm(i, _):
        here = pl.ds(k * own + i * step, step)
        wide = a_s[here, :].astype(jnp.float32)
        scale = lax.rsqrt(jnp.mean(wide * wide, -1, keepdims=True) + 1e-6)
        a_s[here, :] = (wide * scale * gain_s[...].astype(jnp.float32)[None]).astype(jnp.bfloat16)

    with jax.named_scope("norm"):
        lax.fori_loop(0, own // step, norm, None)
    xh = own // 2
    for p in (0, 1):
        src = a_s.at[pl.ds(k * own + p * xh, xh)]
        send(f"xT{p}", src, a_s.at[pl.ds(two + k * own + p * xh, xh)], device("T"))
    send("xP", a_s.at[here_own], a_s.at[here_own], partner)

    oh = orows // 2
    tiles = depth // WIDE
    edges = [n * WIDE for n in (0, tiles * 8 // 18, tiles * 13 // 18, tiles * 16 // 18, tiles)]

    def o_at(s, h, p):
        return full_ref.at[pl.ds(s * orows + h * oh, oh), edges[p] : edges[p + 1]]

    late = {}

    def o_copies(name, p, which):
        h = half if which == "half" else other
        src = wo_ref.at[pl.ds(h * oh, oh), edges[p] : edges[p + 1]]
        return [(f"{'o' if which == 'half' else 'of'}{name}{p}", src, o_at(me, h, p), device(name))]

    def fire(make, *args):
        for entry in make(*args):
            copy_of(*entry).start()
        late[(make.__name__, *args)] = (make, args)

    def o_send(name, p, which="half"):
        fire(o_copies, name, p, which)

    o_send("T", 0)
    o_send("T", 1)

    def w_block(name, dk, h, i):
        _, wide, at = spans[i]
        return w_s.at[w_rows(device(name, dk), h), at : at + wide]

    def w_on(name, dk, i):
        block = w_block(name, dk, half, i)
        recv(f"w{name}{dk}{i}", block)
        if name == "T":
            send(f"wO{dk}{i}", block, block, device("K"))
        send(f"g{name}{dk}{i}", block, block, pair)

    for dk in (0, 1):
        for i in parts["v"]:
            w_on("T", dk, i)
            w_on("K", dk, i)
    w_send("K", "q")
    for dk in (0, 1):
        for i in parts["v"]:
            w_on("O", dk, i)
    for dk in (0, 1):
        w_on("T", dk, 2)
    o_send("K", 0)
    for dk in (0, 1):
        w_on("K", dk, 2)

    def w_ready(part):
        for i in parts[part]:
            _, wide, at = spans[i]
            recv(f"wP{i}", w_s.at[pl.ds(partner * wrows, wrows), at : at + wide])
            own_weights[i].wait()
            for name in "TKO":
                for dk in (0, 1):
                    recv(f"g{name}{dk}{i}", w_block(name, dk, other, i))

    first_half = lax.broadcasted_iota(jnp.int32, (own, HEAD), 1) < HEAD // 2
    pairs = kc // (2 * HEAD)
    pw = 2 * HEAD

    def rotation(place):
        angle = (place + lax.broadcasted_iota(jnp.int32, (own, HEAD), 0)).astype(jnp.float32) * freq_s[...]
        cos, sin = jnp.cos(angle), jnp.sin(angle)
        return cos, jnp.where(first_half, -sin, sin)

    def product(rows, at):
        return _dot(a_s[rows, :], w_s[:, pl.ds(pl.multiple_of(at, pw), pw)], 1, 0).astype(jnp.bfloat16)

    def turned(got, cos, sin):
        wide = got.astype(jnp.float32)
        heads = [wide[:, :HEAD], wide[:, HEAD:]]
        return jnp.concatenate([t * cos + pltpu.roll(t, HEAD // 2, 1) * sin for t in heads], 1).astype(jnp.bfloat16)

    def place_of(slot, core):
        return ((c if slot == 0 else mirror) * 2 + core) * own

    def project_kv(slot, core):
        rows, place = pl.ds(slot * two + core * own, own), place_of(slot, core)
        with jax.named_scope("project_kv"):
            cos, sin = rotation(place)

            def one(b, _):
                kv_s[b, pl.ds(place, own), :pw] = turned(product(rows, b * pw), cos, sin)
                kv_s[b, pl.ds(place, own), pw:] = product(rows, kc + b * pw)

            lax.fori_loop(0, pairs, one, None)

    def project_q(first, last):
        with jax.named_scope("project_q"):

            def some(i, _):
                slot, core = lax.div(i, 2), lax.rem(i, 2)
                rows = pl.ds(i * own, own)
                cos, sin = rotation((jnp.where(slot == 0, c, mirror) * 2 + core) * own)

                def one(b, _):
                    for j in (0, 1):
                        q_s[b, rows, j * pw : (j + 1) * pw] = turned(product(rows, 2 * kc + (2 * b + j) * pw), cos, sin)

                lax.fori_loop(0, pairs, one, None)

            lax.fori_loop(first, last, some, None)

    def kv_rows(chunk, b):
        return kv_s.at[b, pl.ds(chunk * two, two), :]

    def kv_send(slot):
        chunk = c if slot == 0 else mirror
        for b in range(pairs):
            send(f"kv{slot}{b}", kv_rows(chunk, b), kv_rows(chunk, b), device("K"), when=chunk < chips - 1)

    def kv_recv(b):
        recv(f"kv0{b}", kv_rows(mate, b), when=mate < chips - 1)
        recv(f"kv1{b}", kv_rows(across, b), when=across < chips - 1)

    whole_pieces = {(name, p) for name in "TK" for p in (2, 3)}

    def on_copies(name, p):
        piece = o_at(device(name), half, p)
        found = []
        if (name, p) == ("K", 0):
            found.append(("oO0", piece, piece, device("T")))
        if name == "T" and p:
            found.append((f"oO{p}", piece, piece, device("K")))
        if (name, p) not in whole_pieces:
            found.append((f"og{name}{p}", piece, piece, pair))
        return found + [(f"od{name}{p}", piece, piece, partner)]

    def over_copies(name, p):
        piece = o_at(device(name), other, p)
        return [(f"oe{name}{p}", piece, piece, partner)]

    def wo_on(name, p):
        recv(f"o{name}{p}", o_at(device(name), half, p))
        fire(on_copies, name, p)

    def wo_over(name, p):
        recv(f"of{name}{p}" if (name, p) in whole_pieces else f"og{name}{p}", o_at(device(name), other, p))
        fire(over_copies, name, p)

    w_ready("v")
    recv("xP", a_s.at[pl.ds((1 - k) * own, own)])
    project_kv(0, k)
    w_on("O", 0, 2)
    project_kv(0, 1 - k)
    w_on("O", 1, 2)
    kv_send(0)
    send("oP", wo_ref, full_ref.at[pl.ds(me * orows, orows)], partner)
    for p in (0, 1):
        got = a_s.at[pl.ds(two + k * own + p * xh, xh)]
        recv(f"xT{p}", got)
        send(f"xp{p}", got, got, partner)
        if p == 0:
            wo_on("K", 0)
            o_send("T", 2)
            o_send("T", 3)
    project_kv(1, k)
    for p in (0, 1):
        recv(f"xp{p}", a_s.at[pl.ds(two + (1 - k) * own + p * xh, xh)])
    project_kv(1, 1 - k)
    kv_send(1)
    w_ready("q")
    project_q(0, 2)
    wo_on("T", 0)
    project_q(2, 4)
    sent("x", "g", "w")
    keep_wo = pltpu.make_async_copy(wo_ref, a_s.at[pl.ds(2 * own, own)], ls.at[0])
    keep_wo.start()
    load_x = pltpu.make_async_copy(x_ref, a_s.at[pl.ds(0, own)], ls.at[1])
    load_x.start()
    put_wo = pltpu.make_async_copy(a_s.at[pl.ds(2 * own, own)], full_ref.at[pl.ds(me * orows, orows)], ls.at[0])

    scale = HEAD**-0.5
    e = scale * LOG2E
    heads, share = 4, 2
    ones = jnp.ones((8, own), jnp.bfloat16)
    dv = HEAD

    def blocks_before(t):
        b, i = lax.div(t, 3), lax.rem(t, 3)
        far, near = mirror * 2 + 1, c * 2 + 1
        first, second, third, fourth = far + 1 - k, far + k, near + 1 - k, near + k
        done = b * (first + second + third) + jnp.where(i > 0, first, 0) + jnp.where(i > 1, second, 0)
        return jnp.where(t < 6, done, 2 * (first + second + third) + (t - 6) * fourth)

    def attend(slot, core, b, done):
        rows = pl.ds(slot * two + core * own, own)
        block_here = jnp.where(slot == 0, c, mirror) * 2 + core
        top_s[...] = jnp.full(top_s.shape, NEG, jnp.float32)
        mix_s[...] = jnp.zeros(mix_s.shape, jnp.float32)

        def block(j, masked):
            keys = pl.ds(j * own, own)
            scores = []
            for h in range(heads):
                at = (h // share) * HEAD
                scores.append(_dot(kv_s[b, keys, at : at + HEAD], q_s[b, rows, h * HEAD : (h + 1) * HEAD], 1, 1))
            if masked:
                ok = lax.broadcasted_iota(jnp.int32, (own, own), 1) >= lax.broadcasted_iota(jnp.int32, (own, own), 0)
            weights, keeps = [], []
            for h, s in enumerate(scores):
                if masked:
                    s = jnp.where(ok, s, HIDDEN)
                old = top_s[h : h + 1, :]
                top = jnp.maximum(old, s.max(axis=0, keepdims=True))
                top_s[h : h + 1, :] = top
                weights.append(jnp.exp2((s - top) * e).astype(jnp.bfloat16))
                keeps.append(jnp.exp2((old - top) * e))
            for h, (p, keep) in enumerate(zip(weights, keeps)):
                at = pw + (h // share) * HEAD
                values = jnp.concatenate([kv_s[b, keys, at : at + HEAD].T, ones], axis=0)
                mix_s[h] = mix_s[h] * keep + _dot(values, p, 1, 0)

        def whole(j, _):
            events(done + j)
            block(j, False)

        lax.fori_loop(0, block_here, whole, None)
        events(done + block_here)
        block(block_here, True)
        for h in range(heads):
            q_s[b, rows, h * HEAD : (h + 1) * HEAD] = (mix_s[h, :dv, :] * (1 / mix_s[h, dv : dv + 1, :])).T.astype(jnp.bfloat16)

    hc = heads * HEAD
    base = len(ids)
    for i in range(6):
        ids[f"seen{i}"] = base + i

    def spot(t):
        b = jnp.where(t < 6, lax.div(t, 3), t - 6)
        i = jnp.where(t < 6, lax.rem(t, 3), 3)
        slot = jnp.where(i < 2, 1, 0)
        core = lax.rem(k + lax.rem(i + 1, 2), 2)
        return slot, core, b

    def event_at(n):
        if n == 1:
            wo_on("T", 1)
            o_send("K", 1)
        if n == 3:
            wo_over("K", 0)
            keep_wo.wait()
            put_wo.start()
        if n == 11:
            wo_over("T", 0)
        if n == 14:
            wo_on("O", 0)
        if n == 20:
            wo_over("T", 1)
        if n == 22:
            wo_on("T", 2)
            wo_on("T", 3)
            for p in (2, 3):
                o_send("K", p)
                o_send("K", p, "other")
        if n == 25:
            wo_on("O", 1)
        if n == 33:
            wo_on("K", 1)
        if n == 35:
            wo_over("O", 0)

    def events(unit):
        for n in (1, 3, 11, 14, 20, 22, 25, 33, 35):
            pl.when(unit == n)(functools.partial(event_at, n))

    def seen_copy(t, to, src_unit, rows, b):
        return pltpu.make_async_remote_copy(q_s.at[b, rows], seen_s.at[:, pl.ds(pl.multiple_of(src_unit * qc + b * hc, 128), hc)],
                                            ss.at[base + t], rs.at[base + t], device_id={"sp": to}, device_id_type=MESH)

    def attention(t, _):
        slot, core, b = spot(t)
        rows = pl.ds(slot * two + core * own, own)
        pl.when(t == 3)(lambda: kv_recv(1))
        with jax.named_scope("attend"):
            attend(slot, core, b, blocks_before(t))

        @pl.when(t < 6)
        def _():
            to = jnp.where(slot == 0, c, mirror) * 2 + core
            seen_copy(t, to, unit_here, rows, b).start()

        @pl.when(t >= 6)
        def _():
            own_seen(b).start()

    def own_seen(b):
        return pltpu.make_async_copy(q_s.at[b, here_own], seen_s.at[:, pl.ds(pl.multiple_of(unit_here * qc + b * hc, 128), hc)], ls.at[2 + b])

    def o_ready(p):
        for name in "KTO":
            s = device(name, 1)
            recv(f"od{name}{p}", o_at(s, half, p))
            recv(f"oe{name}{p}", o_at(s, other, p))

    slots = (qc + 2 * kc) // WIDE

    def fetch(n):
        slot = lax.rem(n, slots)
        columns = pl.ds(pl.multiple_of(slot * WIDE, 128), WIDE)
        return pltpu.make_async_copy(full_ref.at[:, pl.ds(pl.multiple_of(n * WIDE, 128), WIDE)],
                                     w_s.at[pl.ds(0, full_ref.shape[0]), columns], ls.at[4 + slot])

    def put(n):
        columns = pl.ds(pl.multiple_of(n * WIDE, 128), WIDE)
        return pltpu.make_async_copy(a_s.at[pl.ds(own, own), columns], y_ref.at[:, columns], ls.at[4 + slots])

    def before_tile(at):
        first, second, third = (edges[p] // WIDE for p in (1, 2, 3))
        if at == first:
            o_ready(1)
            fetch_piece(1)
            wo_on("K", 2)
            wo_over("K", 2)
        if at == first + 3:
            wo_over("O", 2)
            wo_over("T", 2)
            wo_on("K", 3)
        if at == first + 4:
            o_ready(2)
            fetch_piece(2)
        if at == second:
            wo_over("K", 3)
            wo_over("T", 3)
            wo_over("O", 3)
        if at == third - 1:
            o_ready(3)
            fetch_piece(3)

    def outputs(first, last):
        def tile(n, _):
            start = edges[1] // WIDE
            for at in (start, start + 3, start + 4, edges[2] // WIDE, edges[3] // WIDE - 1):
                pl.when(n == at)(functools.partial(before_tile, at))
            fetch(n).wait()
            columns = pl.ds(pl.multiple_of(n * WIDE, 128), WIDE)
            slot = pl.ds(pl.multiple_of(lax.rem(n, slots) * WIDE, 128), WIDE)
            got = _dot(seen_s[...], w_s[pl.ds(0, full_ref.shape[0]), slot], 1, 0)
            a_s[pl.ds(own, own), columns] = (a_s[pl.ds(0, own), columns].astype(jnp.float32) + got).astype(jnp.bfloat16)
            put(n).start()

        with jax.named_scope("outputs"):
            lax.fori_loop(first, last, tile, None)

    def fetch_piece(p):
        lax.fori_loop(edges[p] // WIDE, edges[p + 1] // WIDE, lambda n, _: fetch(n).start(), None)

    kv_recv(0)
    lax.fori_loop(0, 8, attention, None)
    o_send("T", 2, "other")
    o_send("T", 3, "other")
    put_wo.wait()
    recv("oP", full_ref.at[pl.ds(partner * orows, orows)])
    o_ready(0)
    fetch_piece(0)

    near_at = lax.div(c, chips // 2) * 2 * qc
    far_at = 2 * qc - near_at
    early = acc_s.shape[1] // WIDE

    def seen_in(t):
        b, i = divmod(t, 3)
        name, dk = ("T", (i + 1) % 2) if i < 2 else ("S", 1)
        with jax.named_scope(f"seen_{t}"):
            seen_copy(t, partner, unit(name, dk), pl.ds(0, own), b).wait_recv()

    def strip(n):
        return pl.ds(pl.multiple_of(n * WIDE, 128), WIDE), pl.ds(pl.multiple_of(lax.rem(n, slots) * WIDE, 128), WIDE)

    def product_of(at, wide, slot):
        here = pl.ds(pl.multiple_of(at, 128), wide)
        return _dot(seen_s[:, here], w_s[here, slot], 1, 0)

    def early_tile(n, _):
        fetch(n).wait()
        columns, slot = strip(n)
        total = product_of(near_at, 2 * qc, slot)
        for u in (0, 1):
            total = total + product_of(far_at + u * qc, hc, slot)
        return total

    def late_tile(n, total):
        columns, slot = strip(n)
        total = total + a_s[pl.ds(0, own), columns].astype(jnp.float32)
        for u in (0, 1):
            total = total + product_of(far_at + u * qc + hc, hc, slot)
        a_s[pl.ds(own, own), columns] = total.astype(jnp.bfloat16)
        put(n).start()

    rows_in = own // heads

    def keep(n, _):
        acc_s[:, strip(n)[0]] = early_tile(n, None)

    def keep_last(i, _):
        total = early_tile(early + i, None)
        for h in range(heads):
            mix_s[h, :rows_in, pl.ds(pl.multiple_of(i * WIDE, 128), WIDE)] = total[h * rows_in : (h + 1) * rows_in]

    def finish(n, _):
        late_tile(n, acc_s[:, strip(n)[0]])

    def finish_last(i, _):
        kept = [mix_s[h, :rows_in, pl.ds(pl.multiple_of(i * WIDE, 128), WIDE)] for h in range(heads)]
        late_tile(early + i, jnp.concatenate(kept, axis=0))

    rest = edges[1] // WIDE - early
    for t in (0, 1, 2, 5):
        seen_in(t)
    for b in (0, 1):
        own_seen(b).wait()
    load_x.wait()
    with jax.named_scope("outputs_early"):
        lax.fori_loop(0, early, keep, None)
        lax.fori_loop(0, rest, keep_last, None)
    wo_over("O", 1)
    wo_on("O", 2)
    wo_on("O", 3)
    for t in (3, 4):
        seen_in(t)
    wo_over("K", 1)
    with jax.named_scope("outputs_late"):
        lax.fori_loop(0, early, finish, None)
        lax.fori_loop(0, rest, finish_last, None)
    outputs(edges[1] // WIDE, tiles)
    for b in (0, 1):
        for i in range(3):
            slot = 1 if i < 2 else 0
            core = lax.rem(k + (i + 1) % 2, 2)
            to = (mirror if slot else c) * 2 + core
            seen_copy(3 * b + i, to, unit_here, pl.ds(slot * two + core * own, own), b).wait_send()
    sent()
    with jax.named_scope("late"):
        for make, args in late.values():
            for entry in make(*args):
                copy_of(*entry).wait_send()
    with jax.named_scope("puts"):
        pltpu.make_async_copy(a_s.at[pl.ds(own, own)], y_ref, ls.at[4 + slots]).wait()


def solution(mesh):
    n_sp = mesh.shape["sp"]

    def step(x, gain, wq, wk, wv, wo):
        own, depth = x.shape
        units = n_sp // 2
        columns = (wq.shape[1] + wk.shape[1] + wv.shape[1]) // units
        half = HEAD // 2
        freq = np.float32(THETA) ** (-np.arange(half, dtype=np.float32) / half)
        freq = jnp.asarray(np.concatenate([freq, freq])[None])
        kc = wk.shape[1] // units
        pairs = kc // (2 * HEAD)
        hbm = pl.BlockSpec(memory_space=pltpu.HBM)
        y, _ = pl.pallas_call(
            functools.partial(_kernel, n_sp),
            out_shape=[jax.ShapeDtypeStruct((own, depth), jnp.bfloat16),
                       jax.ShapeDtypeStruct((wo.shape[0] * n_sp, depth), jnp.bfloat16)],
            in_specs=[hbm] * 7,
            out_specs=[hbm, hbm],
            scratch_shapes=[
                pltpu.VMEM((4 * own, depth), jnp.bfloat16),
                pltpu.VMEM((wq.shape[0] * n_sp, columns), jnp.bfloat16),
                pltpu.VMEM((pairs, 4 * own, 4 * HEAD), jnp.bfloat16),
                pltpu.VMEM((pairs, own * n_sp, 4 * HEAD), jnp.bfloat16),
                pltpu.VMEM((own, wq.shape[1]), jnp.bfloat16),
                pltpu.VMEM((4, own), jnp.float32),
                pltpu.VMEM((4, HEAD + 8, own), jnp.float32),
                pltpu.VMEM((own, depth // 3), jnp.float32),
                pltpu.VMEM(gain.shape, jnp.bfloat16),
                pltpu.VMEM(freq.shape, jnp.float32),
                pltpu.SemaphoreType.DMA((103,)),
                pltpu.SemaphoreType.DMA((103,)),
                pltpu.SemaphoreType.DMA((13,)),
            ],
            compiler_params=pltpu.CompilerParams(collective_id=0, has_side_effects=True, vmem_limit_bytes=VMEM),
        )(x, gain, freq, wq, wk, wv, wo)
        return y

    tokens, whole = P(("dp", "sp"), None), P("sp", None)
    return jax.shard_map(
        step,
        mesh=mesh,
        in_specs=(tokens, P(None), whole, whole, whole, whole),
        out_specs=tokens,
        check_vma=False,
    )
```

```python
import functools

import jax
import jax.numpy as jnp
import numpy as np
from jax import lax
from jax.experimental import pallas as pl
from jax.experimental.pallas import tpu as pltpu
from jax.sharding import PartitionSpec as P

HEAD = 128
THETA = 10000
NEG = -3.3e38
LOG2E = 1.4426950408889634
VMEM = 67043328
MESH = pl.DeviceIdType.MESH
WIDE = 256


def _dot(a, b, ca, cb):
    return lax.dot_general(a, b, (((ca,), (cb,)), ((), ())), preferred_element_type=jnp.float32)


def _kernel(n_sp, x_ref, gain_ref, freq_ref, wq_ref, wk_ref, wv_ref, wo_ref, y_ref, full_ref,
            a_s, w_s, q_s, kv_s, seen_s, top_s, mix_s, acc_s, gain_s, freq_s, ss, rs, ls):
    me, group = lax.axis_index("sp"), lax.axis_index("dp")
    chips = n_sp // 2
    c, k = lax.div(me, 2), lax.rem(me, 2)
    half = lax.rem(group, 2)
    other = 1 - half
    pair = {"dp": group + 1 - 2 * half, "sp": me}
    own, depth = x_ref.shape
    wrows = wq_ref.shape[0]
    hrows = wrows // 2
    orows = wo_ref.shape[0]
    units = chips
    qc, kc = wq_ref.shape[1] // units, wk_ref.shape[1] // units
    two = 2 * own

    mate, mirror = c + 1 - 2 * lax.rem(c, 2), chips - 1 - c
    across = chips - 1 - mate
    chip = {"S": c, "K": mate, "T": mirror, "O": across}

    def device(name, dk=0):
        return chip[name] * 2 + lax.rem(k + dk, 2)

    def unit(name, dk=0):
        return lax.div(chip[name], chips // 2) * 2 + lax.rem(k + dk, 2)

    partner = device("S", 1)
    unit_here = unit("S")

    ids = {}
    started = []

    def copy_of(name, src, dst, to):
        i = ids.setdefault(name, len(ids))
        return pltpu.make_async_remote_copy(src, dst, ss.at[i], rs.at[i], device_id=to if isinstance(to, dict) else {"sp": to},
                                            device_id_type=MESH)

    def send(name, src, dst, to, when=None):
        copy = copy_of(name, src, dst, to)
        if when is None:
            copy.start()
        else:
            pl.when(when)(copy.start)
        started.append((name, copy, when))

    def recv(name, dst, when=None):
        with jax.named_scope(f"recv_{name}"):
            copy = copy_of(name, dst, dst, partner)
            if when is None:
                copy.wait_recv()
            else:
                pl.when(when)(copy.wait_recv)

    def sent(*names):
        with jax.named_scope("sent"):
            for entry in list(started):
                name, copy, when = entry
                if not names or any(name.startswith(n) for n in names):
                    if when is None:
                        copy.wait_send()
                    else:
                        pl.when(when)(copy.wait_send)
                    started.remove(entry)

    barrier = pltpu.get_barrier_semaphore()
    for name in "SKT":
        for dk in (0, 1):
            if (name, dk) != ("S", 0):
                pl.semaphore_signal(barrier, inc=1, device_id={"sp": device(name, dk)}, device_id_type=MESH)
    pl.semaphore_signal(barrier, inc=1, device_id=pair, device_id_type=MESH)
    here_own = pl.ds(k * own, own)
    load_x = pltpu.make_async_copy(x_ref, a_s.at[here_own], ls.at[0])
    load_x.start()
    small = [pltpu.make_async_copy(gain_ref, gain_s, ls.at[5]), pltpu.make_async_copy(freq_ref, freq_s, ls.at[6])]
    for copy in small:
        copy.start()
    spans = ((wk_ref, kc, 0), (wv_ref, kc, kc), (wq_ref, qc, 2 * kc))
    own_weights = []
    for i, (ref, wide, at) in enumerate(spans):
        copy = pltpu.make_async_copy(ref.at[:, pl.ds(pl.multiple_of(unit_here * wide, 128), wide)],
                                     w_s.at[pl.ds(me * wrows, wrows), at : at + wide], ls.at[1 + i])
        copy.start()
        own_weights.append(copy)
    with jax.named_scope("k_barrier"):
        pl.semaphore_wait(barrier, 6)

    def w_rows(s, h):
        return pl.ds(s * wrows + h * hrows, hrows)

    parts = {"v": (0, 1), "q": (2,)}

    def w_send(name, part):
        for dk in (0, 1):
            for i, (ref, wide, at) in enumerate(spans):
                if i in parts[part]:
                    columns = pl.ds(pl.multiple_of(unit(name, dk) * wide, 128), wide)
                    send(f"w{name}{dk}{i}", ref.at[pl.ds(half * hrows, hrows), columns], w_s.at[w_rows(me, half), at : at + wide],
                         device(name, dk))

    w_send("T", "v")
    w_send("K", "v")
    w_send("T", "q")
    for i, (ref, wide, at) in enumerate(spans):
        columns = pl.ds(pl.multiple_of(unit("S", 1) * wide, 128), wide)
        send(f"wP{i}", ref.at[:, columns], w_s.at[pl.ds(me * wrows, wrows), at : at + wide], partner)

    load_x.wait()
    for copy in small:
        copy.wait()
    step = 32

    def norm(i, _):
        here = pl.ds(k * own + i * step, step)
        wide = a_s[here, :].astype(jnp.float32)
        scale = lax.rsqrt(jnp.mean(wide * wide, -1, keepdims=True) + 1e-6)
        a_s[here, :] = (wide * scale * gain_s[...].astype(jnp.float32)[None]).astype(jnp.bfloat16)

    with jax.named_scope("norm"):
        lax.fori_loop(0, own // step, norm, None)
    xh = own // 2
    for p in (0, 1):
        src = a_s.at[pl.ds(k * own + p * xh, xh)]
        send(f"xT{p}", src, a_s.at[pl.ds(two + k * own + p * xh, xh)], device("T"))
    send("xP", a_s.at[here_own], a_s.at[here_own], partner)

    oh = orows // 2
    tiles = depth // WIDE
    edges = [n * WIDE for n in (0, tiles * 8 // 18, tiles * 13 // 18, tiles * 16 // 18, tiles)]

    def o_at(s, h, p):
        return full_ref.at[pl.ds(s * orows + h * oh, oh), edges[p] : edges[p + 1]]

    late = {}

    def o_copies(name, p, which):
        h = half if which == "half" else other
        src = wo_ref.at[pl.ds(h * oh, oh), edges[p] : edges[p + 1]]
        return [(f"{'o' if which == 'half' else 'of'}{name}{p}", src, o_at(me, h, p), device(name))]

    def fire(make, *args):
        for entry in make(*args):
            copy_of(*entry).start()
        late[(make.__name__, *args)] = (make, args)

    def o_send(name, p, which="half"):
        fire(o_copies, name, p, which)

    o_send("T", 0)
    o_send("T", 1)

    def w_block(name, dk, h, i):
        _, wide, at = spans[i]
        return w_s.at[w_rows(device(name, dk), h), at : at + wide]

    def w_on(name, dk, i):
        block = w_block(name, dk, half, i)
        recv(f"w{name}{dk}{i}", block)
        if name == "T":
            send(f"wO{dk}{i}", block, block, device("K"))
        send(f"g{name}{dk}{i}", block, block, pair)

    for dk in (0, 1):
        for i in parts["v"]:
            w_on("T", dk, i)
            w_on("K", dk, i)
    w_send("K", "q")
    for dk in (0, 1):
        for i in parts["v"]:
            w_on("O", dk, i)
    for dk in (0, 1):
        w_on("T", dk, 2)
    o_send("K", 0)
    for dk in (0, 1):
        w_on("K", dk, 2)

    def w_ready(part):
        for i in parts[part]:
            _, wide, at = spans[i]
            recv(f"wP{i}", w_s.at[pl.ds(partner * wrows, wrows), at : at + wide])
            own_weights[i].wait()
            for name in "TKO":
                for dk in (0, 1):
                    recv(f"g{name}{dk}{i}", w_block(name, dk, other, i))

    first_half = lax.broadcasted_iota(jnp.int32, (own, HEAD), 1) < HEAD // 2
    pairs = kc // (2 * HEAD)
    pw = 2 * HEAD

    def rotation(place):
        angle = (place + lax.broadcasted_iota(jnp.int32, (own, HEAD), 0)).astype(jnp.float32) * freq_s[...]
        cos, sin = jnp.cos(angle), jnp.sin(angle)
        return cos, jnp.where(first_half, -sin, sin)

    def product(rows, at):
        return _dot(a_s[rows, :], w_s[:, pl.ds(pl.multiple_of(at, pw), pw)], 1, 0).astype(jnp.bfloat16)

    def turned(got, cos, sin):
        wide = got.astype(jnp.float32)
        heads = [wide[:, :HEAD], wide[:, HEAD:]]
        return jnp.concatenate([t * cos + pltpu.roll(t, HEAD // 2, 1) * sin for t in heads], 1).astype(jnp.bfloat16)

    def place_of(slot, core):
        return ((c if slot == 0 else mirror) * 2 + core) * own

    def project_kv(slot, core):
        rows, place = pl.ds(slot * two + core * own, own), place_of(slot, core)
        with jax.named_scope("project_kv"):
            cos, sin = rotation(place)

            def one(b, _):
                kv_s[b, pl.ds(place, own), :pw] = turned(product(rows, b * pw), cos, sin)
                kv_s[b, pl.ds(place, own), pw:] = product(rows, kc + b * pw)

            lax.fori_loop(0, pairs, one, None)

    def project_q(first, last):
        with jax.named_scope("project_q"):

            def some(i, _):
                slot, core = lax.div(i, 2), lax.rem(i, 2)
                rows = pl.ds(i * own, own)
                cos, sin = rotation((jnp.where(slot == 0, c, mirror) * 2 + core) * own)

                def one(b, _):
                    for j in (0, 1):
                        q_s[b, rows, j * pw : (j + 1) * pw] = turned(product(rows, 2 * kc + (2 * b + j) * pw), cos, sin)

                lax.fori_loop(0, pairs, one, None)

            lax.fori_loop(first, last, some, None)

    def kv_rows(chunk, b):
        return kv_s.at[b, pl.ds(chunk * two, two), :]

    def kv_send(slot):
        chunk = c if slot == 0 else mirror
        for b in range(pairs):
            send(f"kv{slot}{b}", kv_rows(chunk, b), kv_rows(chunk, b), device("K"), when=chunk < chips - 1)

    def kv_recv(b):
        recv(f"kv0{b}", kv_rows(mate, b), when=mate < chips - 1)
        recv(f"kv1{b}", kv_rows(across, b), when=across < chips - 1)

    whole_pieces = {(name, p) for name in "TK" for p in (2, 3)}

    def on_copies(name, p):
        piece = o_at(device(name), half, p)
        found = []
        if (name, p) == ("K", 0):
            found.append(("oO0", piece, piece, device("T")))
        if name == "T" and p:
            found.append((f"oO{p}", piece, piece, device("K")))
        if (name, p) not in whole_pieces:
            found.append((f"og{name}{p}", piece, piece, pair))
        return found + [(f"od{name}{p}", piece, piece, partner)]

    def over_copies(name, p):
        piece = o_at(device(name), other, p)
        return [(f"oe{name}{p}", piece, piece, partner)]

    def wo_on(name, p):
        recv(f"o{name}{p}", o_at(device(name), half, p))
        fire(on_copies, name, p)

    def wo_over(name, p):
        recv(f"of{name}{p}" if (name, p) in whole_pieces else f"og{name}{p}", o_at(device(name), other, p))
        fire(over_copies, name, p)

    w_ready("v")
    recv("xP", a_s.at[pl.ds((1 - k) * own, own)])
    project_kv(0, k)
    w_on("O", 0, 2)
    project_kv(0, 1 - k)
    w_on("O", 1, 2)
    kv_send(0)
    send("oP", wo_ref, full_ref.at[pl.ds(me * orows, orows)], partner)
    for p in (0, 1):
        got = a_s.at[pl.ds(two + k * own + p * xh, xh)]
        recv(f"xT{p}", got)
        send(f"xp{p}", got, got, partner)
        if p == 0:
            wo_on("K", 0)
            o_send("T", 2)
            o_send("T", 3)
    project_kv(1, k)
    for p in (0, 1):
        recv(f"xp{p}", a_s.at[pl.ds(two + (1 - k) * own + p * xh, xh)])
    project_kv(1, 1 - k)
    kv_send(1)
    w_ready("q")
    project_q(0, 2)
    wo_on("T", 0)
    project_q(2, 4)
    sent("x", "g", "w")
    keep_wo = pltpu.make_async_copy(wo_ref, a_s.at[pl.ds(2 * own, own)], ls.at[0])
    keep_wo.start()
    load_x = pltpu.make_async_copy(x_ref, a_s.at[pl.ds(0, own)], ls.at[1])
    load_x.start()
    put_wo = pltpu.make_async_copy(a_s.at[pl.ds(2 * own, own)], full_ref.at[pl.ds(me * orows, orows)], ls.at[0])

    scale = HEAD**-0.5
    e = scale * LOG2E
    heads, share = 4, 2
    ones = jnp.ones((8, own), jnp.bfloat16)
    dv = HEAD

    def blocks_before(t):
        b, i = lax.div(t, 3), lax.rem(t, 3)
        far, near = mirror * 2 + 1, c * 2 + 1
        first, second, third, fourth = far + 1 - k, far + k, near + 1 - k, near + k
        done = b * (first + second + third) + jnp.where(i > 0, first, 0) + jnp.where(i > 1, second, 0)
        return jnp.where(t < 6, done, 2 * (first + second + third) + (t - 6) * fourth)

    def attend(slot, core, b, done):
        rows = pl.ds(slot * two + core * own, own)
        block_here = jnp.where(slot == 0, c, mirror) * 2 + core
        top_s[...] = jnp.full(top_s.shape, NEG, jnp.float32)
        mix_s[...] = jnp.zeros(mix_s.shape, jnp.float32)

        def block(j, masked):
            keys = pl.ds(j * own, own)
            scores = []
            for h in range(heads):
                at = (h // share) * HEAD
                scores.append(_dot(kv_s[b, keys, at : at + HEAD], q_s[b, rows, h * HEAD : (h + 1) * HEAD], 1, 1))
            if masked:
                ok = lax.broadcasted_iota(jnp.int32, (own, own), 1) >= lax.broadcasted_iota(jnp.int32, (own, own), 0)
            weights, keeps = [], []
            for h, s in enumerate(scores):
                if masked:
                    s = jnp.where(ok, s, NEG)
                old = top_s[h : h + 1, :]
                top = jnp.maximum(old, s.max(axis=0, keepdims=True))
                top_s[h : h + 1, :] = top
                weights.append(jnp.exp2((s - top) * e).astype(jnp.bfloat16))
                keeps.append(jnp.exp2((old - top) * e))
            for h, (p, keep) in enumerate(zip(weights, keeps)):
                at = pw + (h // share) * HEAD
                values = jnp.concatenate([kv_s[b, keys, at : at + HEAD].T, ones], axis=0)
                mix_s[h] = mix_s[h] * keep + _dot(values, p, 1, 0)

        def whole(j, _):
            events(done + j)
            block(j, False)

        lax.fori_loop(0, block_here, whole, None)
        events(done + block_here)
        block(block_here, True)
        for h in range(heads):
            q_s[b, rows, h * HEAD : (h + 1) * HEAD] = (mix_s[h, :dv, :] * (1 / mix_s[h, dv : dv + 1, :])).T.astype(jnp.bfloat16)

    hc = heads * HEAD
    base = len(ids)
    for i in range(6):
        ids[f"seen{i}"] = base + i

    def spot(t):
        b = jnp.where(t < 6, lax.div(t, 3), t - 6)
        i = jnp.where(t < 6, lax.rem(t, 3), 3)
        slot = jnp.where(i < 2, 1, 0)
        core = lax.rem(k + lax.rem(i + 1, 2), 2)
        return slot, core, b

    def event_at(n):
        if n == 1:
            wo_on("T", 1)
            o_send("K", 1)
        if n == 3:
            wo_over("K", 0)
            keep_wo.wait()
            put_wo.start()
        if n == 11:
            wo_over("T", 0)
        if n == 14:
            wo_on("O", 0)
        if n == 20:
            wo_over("T", 1)
        if n == 22:
            wo_on("T", 2)
            wo_on("T", 3)
            for p in (2, 3):
                o_send("K", p)
                o_send("K", p, "other")
        if n == 25:
            wo_on("O", 1)
        if n == 33:
            wo_on("K", 1)
        if n == 35:
            wo_over("O", 0)

    def events(unit):
        for n in (1, 3, 11, 14, 20, 22, 25, 33, 35):
            pl.when(unit == n)(functools.partial(event_at, n))

    def seen_copy(t, to, src_unit, rows, b):
        return pltpu.make_async_remote_copy(q_s.at[b, rows], seen_s.at[:, pl.ds(pl.multiple_of(src_unit * qc + b * hc, 128), hc)],
                                            ss.at[base + t], rs.at[base + t], device_id={"sp": to}, device_id_type=MESH)

    def attention(t, _):
        slot, core, b = spot(t)
        rows = pl.ds(slot * two + core * own, own)
        pl.when(t == 3)(lambda: kv_recv(1))
        with jax.named_scope("attend"):
            attend(slot, core, b, blocks_before(t))

        @pl.when(t < 6)
        def _():
            to = jnp.where(slot == 0, c, mirror) * 2 + core
            seen_copy(t, to, unit_here, rows, b).start()

        @pl.when(t >= 6)
        def _():
            own_seen(b).start()

    def own_seen(b):
        return pltpu.make_async_copy(q_s.at[b, here_own], seen_s.at[:, pl.ds(pl.multiple_of(unit_here * qc + b * hc, 128), hc)], ls.at[2 + b])

    def o_ready(p):
        for name in "KTO":
            s = device(name, 1)
            recv(f"od{name}{p}", o_at(s, half, p))
            recv(f"oe{name}{p}", o_at(s, other, p))

    slots = (qc + 2 * kc) // WIDE

    def fetch(n):
        slot = lax.rem(n, slots)
        columns = pl.ds(pl.multiple_of(slot * WIDE, 128), WIDE)
        return pltpu.make_async_copy(full_ref.at[:, pl.ds(pl.multiple_of(n * WIDE, 128), WIDE)],
                                     w_s.at[pl.ds(0, full_ref.shape[0]), columns], ls.at[4 + slot])

    def put(n):
        columns = pl.ds(pl.multiple_of(n * WIDE, 128), WIDE)
        return pltpu.make_async_copy(a_s.at[pl.ds(own, own), columns], y_ref.at[:, columns], ls.at[4 + slots])

    def before_tile(at):
        first, second, third = (edges[p] // WIDE for p in (1, 2, 3))
        if at == first:
            o_ready(1)
            fetch_piece(1)
            wo_on("K", 2)
            wo_over("K", 2)
        if at == first + 3:
            wo_over("O", 2)
            wo_over("T", 2)
            wo_on("K", 3)
        if at == first + 4:
            o_ready(2)
            fetch_piece(2)
        if at == second:
            wo_over("K", 3)
            wo_over("T", 3)
            wo_over("O", 3)
        if at == third - 1:
            o_ready(3)
            fetch_piece(3)

    def outputs(first, last):
        def tile(n, _):
            start = edges[1] // WIDE
            for at in (start, start + 3, start + 4, edges[2] // WIDE, edges[3] // WIDE - 1):
                pl.when(n == at)(functools.partial(before_tile, at))
            fetch(n).wait()
            columns = pl.ds(pl.multiple_of(n * WIDE, 128), WIDE)
            slot = pl.ds(pl.multiple_of(lax.rem(n, slots) * WIDE, 128), WIDE)
            got = _dot(seen_s[...], w_s[pl.ds(0, full_ref.shape[0]), slot], 1, 0)
            a_s[pl.ds(own, own), columns] = (a_s[pl.ds(0, own), columns].astype(jnp.float32) + got).astype(jnp.bfloat16)
            put(n).start()

        with jax.named_scope("outputs"):
            lax.fori_loop(first, last, tile, None)

    def fetch_piece(p):
        lax.fori_loop(edges[p] // WIDE, edges[p + 1] // WIDE, lambda n, _: fetch(n).start(), None)

    kv_recv(0)
    lax.fori_loop(0, 8, attention, None)
    o_send("T", 2, "other")
    o_send("T", 3, "other")
    put_wo.wait()
    recv("oP", full_ref.at[pl.ds(partner * orows, orows)])
    o_ready(0)
    fetch_piece(0)

    near_at = lax.div(c, chips // 2) * 2 * qc
    far_at = 2 * qc - near_at
    early = acc_s.shape[1] // WIDE

    def seen_in(t):
        b, i = divmod(t, 3)
        name, dk = ("T", (i + 1) % 2) if i < 2 else ("S", 1)
        with jax.named_scope(f"seen_{t}"):
            seen_copy(t, partner, unit(name, dk), pl.ds(0, own), b).wait_recv()

    def strip(n):
        return pl.ds(pl.multiple_of(n * WIDE, 128), WIDE), pl.ds(pl.multiple_of(lax.rem(n, slots) * WIDE, 128), WIDE)

    def product_of(at, wide, slot):
        here = pl.ds(pl.multiple_of(at, 128), wide)
        return _dot(seen_s[:, here], w_s[here, slot], 1, 0)

    def early_tile(n, _):
        fetch(n).wait()
        columns, slot = strip(n)
        total = product_of(near_at, 2 * qc, slot)
        for u in (0, 1):
            total = total + product_of(far_at + u * qc, hc, slot)
        return total

    def late_tile(n, total):
        columns, slot = strip(n)
        total = total + a_s[pl.ds(0, own), columns].astype(jnp.float32)
        for u in (0, 1):
            total = total + product_of(far_at + u * qc + hc, hc, slot)
        a_s[pl.ds(own, own), columns] = total.astype(jnp.bfloat16)
        put(n).start()

    rows_in = own // heads

    def keep(n, _):
        acc_s[:, strip(n)[0]] = early_tile(n, None)

    def keep_last(i, _):
        total = early_tile(early + i, None)
        for h in range(heads):
            mix_s[h, :rows_in, pl.ds(pl.multiple_of(i * WIDE, 128), WIDE)] = total[h * rows_in : (h + 1) * rows_in]

    def finish(n, _):
        late_tile(n, acc_s[:, strip(n)[0]])

    def finish_last(i, _):
        kept = [mix_s[h, :rows_in, pl.ds(pl.multiple_of(i * WIDE, 128), WIDE)] for h in range(heads)]
        late_tile(early + i, jnp.concatenate(kept, axis=0))

    rest = edges[1] // WIDE - early
    for t in (0, 1, 2, 5):
        seen_in(t)
    for b in (0, 1):
        own_seen(b).wait()
    load_x.wait()
    with jax.named_scope("outputs_early"):
        lax.fori_loop(0, early, keep, None)
        lax.fori_loop(0, rest, keep_last, None)
    wo_over("O", 1)
    wo_on("O", 2)
    wo_on("O", 3)
    for t in (3, 4):
        seen_in(t)
    wo_over("K", 1)
    with jax.named_scope("outputs_late"):
        lax.fori_loop(0, early, finish, None)
        lax.fori_loop(0, rest, finish_last, None)
    outputs(edges[1] // WIDE, tiles)
    for b in (0, 1):
        for i in range(3):
            slot = 1 if i < 2 else 0
            core = lax.rem(k + (i + 1) % 2, 2)
            to = (mirror if slot else c) * 2 + core
            seen_copy(3 * b + i, to, unit_here, pl.ds(slot * two + core * own, own), b).wait_send()
    sent()
    with jax.named_scope("late"):
        for make, args in late.values():
            for entry in make(*args):
                copy_of(*entry).wait_send()
    with jax.named_scope("puts"):
        pltpu.make_async_copy(a_s.at[pl.ds(own, own)], y_ref, ls.at[4 + slots]).wait()


def solution(mesh):
    n_sp = mesh.shape["sp"]

    def step(x, gain, wq, wk, wv, wo):
        own, depth = x.shape
        units = n_sp // 2
        columns = (wq.shape[1] + wk.shape[1] + wv.shape[1]) // units
        half = HEAD // 2
        freq = np.float32(THETA) ** (-np.arange(half, dtype=np.float32) / half)
        freq = jnp.asarray(np.concatenate([freq, freq])[None])
        kc = wk.shape[1] // units
        pairs = kc // (2 * HEAD)
        hbm = pl.BlockSpec(memory_space=pltpu.HBM)
        y, _ = pl.pallas_call(
            functools.partial(_kernel, n_sp),
            out_shape=[jax.ShapeDtypeStruct((own, depth), jnp.bfloat16),
                       jax.ShapeDtypeStruct((wo.shape[0] * n_sp, depth), jnp.bfloat16)],
            in_specs=[hbm] * 7,
            out_specs=[hbm, hbm],
            scratch_shapes=[
                pltpu.VMEM((4 * own, depth), jnp.bfloat16),
                pltpu.VMEM((wq.shape[0] * n_sp, columns), jnp.bfloat16),
                pltpu.VMEM((pairs, 4 * own, 4 * HEAD), jnp.bfloat16),
                pltpu.VMEM((pairs, own * n_sp, 4 * HEAD), jnp.bfloat16),
                pltpu.VMEM((own, wq.shape[1]), jnp.bfloat16),
                pltpu.VMEM((4, own), jnp.float32),
                pltpu.VMEM((4, HEAD + 8, own), jnp.float32),
                pltpu.VMEM((own, depth // 3), jnp.float32),
                pltpu.VMEM(gain.shape, jnp.bfloat16),
                pltpu.VMEM(freq.shape, jnp.float32),
                pltpu.SemaphoreType.DMA((103,)),
                pltpu.SemaphoreType.DMA((103,)),
                pltpu.SemaphoreType.DMA((13,)),
            ],
            compiler_params=pltpu.CompilerParams(collective_id=0, has_side_effects=True, vmem_limit_bytes=VMEM),
        )(x, gain, freq, wq, wk, wv, wo)
        return y

    tokens, whole = P(("dp", "sp"), None), P("sp", None)
    return jax.shard_map(
        step,
        mesh=mesh,
        in_specs=(tokens, P(None), whole, whole, whole, whole),
        out_specs=tokens,
        check_vma=False,
    )
```
